32 devices in a mesh: groups: 2 (over x), tile: 16 (over z, y, core).
Axes of the slice: x: 2, y: 2, z: 4, core: 2. Of those that a mesh axis runs over, the one named last changes fastest.
Arguments:
- tracer: float32 [32, 6, 8, 128, 128], P(('groups', 'tile')), parts along dimension 0, may hold values from -6 to 6
- courant_east: bfloat16 [32, 6, 8, 128, 128], P(('groups', 'tile')), parts along dimension 0, may hold values from -1.5 to 1.5
- courant_north: bfloat16 [32, 6, 8, 128, 128], P(('groups', 'tile')), parts along dimension 0, may hold values from -1.5 to 1.5
- diffusivity: bfloat16 [32, 6, 8, 128, 128], P(('groups', 'tile')), parts along dimension 0, may hold values from 0.049804688 to 5
- seam_table: int32 [6, 4, 3], replicated, may hold values from 0 to 5, as said below
Outputs:
- updated: float32 [32, 6, 8, 128, 128], P(('groups', 'tile')), parts along dimension 0
The draws below stay inside these ranges and needn't reach their ends.
There are 2 independent parts, one for each index of `groups`. The reference program is written for one: setup_inputs(seed, part) draws one part's arguments, and reference() takes and returns one part's arrays. A program takes and returns all parts, laid end to end along the dimension named above; an argument that names none is the same for every part. Nothing has to cross between parts.
Inputs may be any that keep to these rules, and one draw needn't show every extreme that they name: seam_table[p, e] = (q, f, r) names the edge f of panel q != p that borders edge e of panel p, and r is 1 where their edge indices run in opposite directions, 0 otherwise; the 24 edges form 12 pairs whose entries name each other with the same r, as on the faces of a cube ; edge 3 of panel 0 borders edge 3 of panel 1.
All inputs are finite; a program needn't handle non-finite values.
Results may differ from the reference program's by a relative error of at most 0.0003.
Values sent between devices are 32-bit elements; how exact they have to be, the bound alone decides.
A program may use at most 128 MiB of HBM per device.

```python
import math
import jax
import jax.numpy as jnp
from jax import lax

CT = 128
LEVELS = 8
PANELS = 6
DEPTH = 2
SIDE = 4
N_TILE = 16


def turn_axes(first_old, second_old, quarter):
    first_axis = jnp.where(quarter == 0, first_old, jnp.where(quarter == 1, second_old, jnp.where(quarter == 2, -first_old, -second_old)))
    second_axis = jnp.where(quarter == 0, second_old, jnp.where(quarter == 1, -first_old, jnp.where(quarter == 2, -second_old, first_old)))
    return (first_axis, second_axis)


def draw_seam_table(key, part):
    normals = jnp.array([[1, 0, 0], [0, 1, 0], [0, 0, 1], [-1, 0, 0], [0, -1, 0], [0, 0, -1]], jnp.int32)
    firsts = jnp.array([[0, 1, 0], [0, 0, 1], [1, 0, 0], [0, 0, 1], [1, 0, 0], [0, 1, 0]], jnp.int32)
    seconds = jnp.array([[0, 0, 1], [1, 0, 0], [0, 1, 0], [0, 1, 0], [0, 0, 1], [1, 0, 0]], jnp.int32)
    split_keys = jax.random.split(jax.random.fold_in(key, 11), 3)
    head_label = jax.random.randint(split_keys[0], (1,), 0, 6)
    quarter = jax.random.randint(split_keys[1], (6, 1), 0, 4)
    centre_zero = normals[head_label]
    first_zero, second_zero = turn_axes(firsts[head_label], seconds[head_label], quarter[0:1])
    centre_one = -first_zero
    first_one = -centre_zero
    second_one = -second_zero
    remaining = jnp.concatenate([-centre_zero, first_zero, second_zero, -second_zero], axis=0)
    remaining = remaining[jax.random.permutation(split_keys[2], 4)]
    same_face = jnp.all(remaining[:, None, :] == normals[None, :, :], axis=-1).astype(jnp.int32)
    rest_labels = jnp.sum(same_face * jnp.arange(6, dtype=jnp.int32)[None, :], axis=1)
    first_rest, second_rest = turn_axes(firsts[rest_labels], seconds[rest_labels], quarter[2:])
    centre = jnp.concatenate([centre_zero, centre_one, remaining], axis=0)
    first_axis = jnp.concatenate([first_zero, first_one, first_rest], axis=0)
    second_axis = jnp.concatenate([second_zero, second_one, second_rest], axis=0)
    middle = jnp.stack([centre - second_axis, centre + first_axis, centre + second_axis, centre - first_axis], axis=1).reshape(24, 3)
    heading = jnp.stack([first_axis, second_axis, first_axis, second_axis], axis=1).reshape(24, 3)
    panel_of = jnp.arange(24, dtype=jnp.int32) // 4
    matches = jnp.all(middle[:, None, :] == middle[None, :, :], axis=-1) & (panel_of[:, None] != panel_of[None, :])
    partner = jnp.sum(matches.astype(jnp.int32) * jnp.arange(24, dtype=jnp.int32)[None, :], axis=1)
    partner_heading = jnp.sum(matches.astype(jnp.int32)[:, :, None] * heading[None, :, :], axis=1)
    reversal = (jnp.sum(heading * partner_heading, axis=-1) < 0).astype(jnp.int32)
    return jnp.stack([partner // 4, partner % 4, reversal], axis=-1).reshape(6, 4, 3).astype(jnp.int32)


def steps_of(key, extent, pieces, least, top_value):
    factor_of = 1.0
    for position, blocks in pieces:
        heights = jax.random.uniform(jax.random.fold_in(jax.random.fold_in(key, 6), position), (blocks,), jnp.float32, least / len(pieces), top_value / len(pieces))
        factor_of = factor_of * jnp.repeat(jnp.exp(heights), extent[position] // blocks).reshape((-1,) + (1,) * (len(extent) - 1 - position))
    return factor_of


def bell_draw(own_key, shape, width, limit, cuts=(), held_as=jnp.bfloat16):
    result = jax.random.normal(own_key, shape, jnp.float32) * width
    if len(cuts) > 0:
        result = steps_of(own_key, shape, cuts, -0.22, 0.18) * result
    return jnp.clip(result, min=-limit, max=limit).astype(held_as)


def setup_inputs(seed: int = 0, part: int = 0) -> dict:
    arg_keys = jax.random.split(jax.random.key(seed), 6)
    own_keys = jax.random.split(jax.random.fold_in(arg_keys[5], part), 6)
    tracer = bell_draw(own_keys[0], (N_TILE, PANELS, LEVELS, CT, CT), 1.0, 6.0, ((0, 16),), jnp.float32)
    courant_east = bell_draw(own_keys[1], (N_TILE, PANELS, LEVELS, CT, CT), 0.3, 1.5, ((0, 16),))
    courant_north = bell_draw(own_keys[2], (N_TILE, PANELS, LEVELS, CT, CT), 0.3, 1.5, ((0, 16),))
    diffusivity = jnp.clip(jnp.exp(math.log(5.0) - 4.609084 * jax.random.uniform(own_keys[3], (N_TILE, PANELS, LEVELS, CT, CT), jnp.float32) ** steps_of(own_keys[3], (N_TILE, PANELS, LEVELS, CT, CT), ((0, 16),), -0.2, 0.2)), 0.049804688, 5.0).astype(jnp.bfloat16)
    seam_table = draw_seam_table(jax.random.fold_in(arg_keys[5], 71), part)
    return dict(tracer=tracer, courant_east=courant_east, courant_north=courant_north, diffusivity=diffusivity, seam_table=seam_table)


def edge_strips(panels, rows_deep):
    south_rows = jnp.moveaxis(panels[:, :, :, :rows_deep], 3, 1)
    east_rows = jnp.moveaxis(panels[:, :, ::-1, :][:, :, :rows_deep, :], 2, 1)
    north_rows = jnp.moveaxis(panels[:, :, :, ::-1][:, :, :, :rows_deep], 3, 1)
    west_rows = jnp.moveaxis(panels[:, :, :rows_deep, :], 2, 1)
    return jnp.stack([south_rows, east_rows, north_rows, west_rows], axis=1)


def centered(extended, along):
    kept = extended.shape[along] - 4

    def shifted(offset):
        return lax.slice_in_dim(extended, 2 + offset, 2 + offset + kept, axis=along)

    return (8.0 * (shifted(1) - shifted(-1)) - (shifted(2) - shifted(-2))) / 12.0


def advance(panels, ghosts, courant_east, courant_north, diffusivity):
    west_part = jnp.moveaxis(ghosts[:, 3, ::-1], 1, 2)
    east_part = jnp.moveaxis(ghosts[:, 1], 1, 2)
    south_part = jnp.transpose(ghosts[:, 0, ::-1], (0, 2, 3, 1))
    north_part = jnp.transpose(ghosts[:, 2], (0, 2, 3, 1))
    along_first = jnp.concatenate([west_part, panels, east_part], axis=2)
    along_second = jnp.concatenate([south_part, panels, north_part], axis=3)
    forced = panels - (courant_east.astype(jnp.float32) * centered(along_first, 2)
                       + courant_north.astype(jnp.float32) * centered(along_second, 3))
    coupling = diffusivity.astype(jnp.float32)
    ratios = []
    partial_values = []
    for height in range(panels.shape[1]):
        diagonal = 1.0 + coupling[:, height]
        if height > 0:
            below = coupling[:, height - 1]
            pivot_value = diagonal + below - below * ratios[-1]
            current = (forced[:, height] + below * partial_values[-1]) / pivot_value
        else:
            pivot_value = diagonal
            current = forced[:, height] / pivot_value
        ratios.append(coupling[:, height] / pivot_value)
        partial_values.append(current)
    solved = [partial_values[-1]]
    for height in range(panels.shape[1] - 2, -1, -1):
        solved.insert(0, partial_values[height] + ratios[height] * solved[0])
    return jnp.stack(solved, axis=1)


def panel_offset(panel_no):
    return (panel_no % 2) * (SIDE * SIDE // 2 + 1)


def to_panels(tiles):
    aligned = jnp.stack([jnp.roll(tiles[:, panel_no], -panel_offset(panel_no), axis=0)
                         for panel_no in range(PANELS)], axis=1)
    shaped = aligned.reshape(SIDE, SIDE, PANELS, LEVELS, CT, CT)
    shaped = jnp.transpose(shaped, (2, 3, 0, 4, 1, 5))
    return shaped.reshape(PANELS, LEVELS, SIDE * CT, SIDE * CT)


def to_tiles(panels):
    shaped = panels.reshape(PANELS, LEVELS, SIDE, CT, SIDE, CT)
    shaped = jnp.transpose(shaped, (2, 4, 0, 1, 3, 5))
    aligned = shaped.reshape(SIDE * SIDE, PANELS, LEVELS, CT, CT)
    return jnp.stack([jnp.roll(aligned[:, panel_no], panel_offset(panel_no), axis=0)
                      for panel_no in range(PANELS)], axis=1)


def reference(tracer, courant_east, courant_north, diffusivity, seam_table):
    panels = to_panels(tracer)
    strips = edge_strips(panels, DEPTH)
    flat_strips = strips.reshape((PANELS * 4,) + strips.shape[2:])
    source_block = (seam_table[:, :, 0] * 4 + seam_table[:, :, 1]).reshape(-1).astype(jnp.int32)
    reverse_it = (seam_table[:, :, 2] == 1).reshape(-1)
    picked = jnp.take(flat_strips, source_block, axis=0)
    picked = jnp.where(reverse_it[:, None, None, None], picked[..., ::-1], picked)
    ghosts = picked.reshape(strips.shape)
    updated = advance(panels, ghosts, to_panels(courant_east), to_panels(courant_north), to_panels(diffusivity))
    return to_tiles(updated)
```

```python
import functools
import math

import jax
import jax.numpy as jnp
from jax import lax
from jax.experimental import pallas as pl
from jax.experimental.pallas import tpu as pltpu
from jax.sharding import PartitionSpec as P

DEPTH = 2
HUBS = 4
VMEM_LIMIT = 59 * 1024 * 1024


def tile_of(device, parity, total):
    return lax.rem(device + total - parity * (total // 2 + 1) + total, total)


def edge_state(device, parity, total, across):
    tile = tile_of(device, parity, total)
    row, col = tile // across, lax.rem(tile, across)
    on = (col == 0, row == across - 1, col == across - 1, row == 0)
    return on, (row, col, row, col)


def edge_tile(edge, spot, across):
    return (spot * across, (across - 1) * across + spot, spot * across + across - 1, spot)[edge]


def central(q, p, k, start, size):
    ct = q.shape[2]
    mid = q[p, k, start:start + size]
    none = jnp.zeros((DEPTH, 128), jnp.float32)
    if start == 0:
        ext = jnp.concatenate([none, q[p, k, 0:size + DEPTH]], axis=0)
        near = [ext[o:o + size] for o in (0, 1, 3, 4)]
    elif start + size == ct:
        ext = jnp.concatenate([q[p, k, start - DEPTH:ct], none], axis=0)
        near = [ext[o:o + size] for o in (0, 1, 3, 4)]
    else:
        near = [q[p, k, start + o:start + o + size] for o in (-2, -1, 1, 2)]
    along_i = 8.0 * (near[2] - near[1]) - (near[3] - near[0])
    along_j = 8.0 * (pltpu.roll(mid, 127, 1) - pltpu.roll(mid, 1, 1)) - (
        pltpu.roll(mid, 126, 1) - pltpu.roll(mid, 2, 1))
    return mid, along_i, along_j


def factors(coupling, levels):
    inverses, ratios, below = [], [], None
    for k in range(levels):
        here = coupling(k)
        if k == 0:
            inverse = 1.0 / (1.0 + here)
        else:
            inverse = 1.0 / ((1.0 + here) + below * (1.0 - ratios[-1]))
        inverses.append(inverse)
        ratios.append(here * inverse)
        below = here
    return inverses, ratios


def solve(forced, coupling, levels):
    ratios, partials = [], []
    for k in range(levels):
        value, here = forced(k), coupling(k)
        if k == 0:
            inverse = 1.0 / (1.0 + here)
            current = value * inverse
        else:
            inverse = 1.0 / ((1.0 + here) + below * (1.0 - ratios[-1]))
            current = (value + below * partials[-1]) * inverse
        ratios.append(here * inverse)
        partials.append(current)
        below = here
    solved = [partials[-1]]
    for k in range(levels - 2, -1, -1):
        solved.insert(0, partials[k] + ratios[k] * solved[0])
    return solved


def update_panel(q, east, north, coupling, u, p):
    _, levels, ct, _ = q.shape
    size = 16
    for start in range(0, ct, size):
        part = pl.ds(start, size)

        def forced(k):
            mid, along_i, along_j = central(q, p, k, start, size)
            return mid - (east[p, k, part].astype(jnp.float32) * along_i
                          + north[p, k, part].astype(jnp.float32) * along_j) * (1.0 / 12.0)

        solved = solve(forced, lambda k: coupling[p, k, part].astype(jnp.float32), levels)
        for k in range(levels):
            u[p, k, part] = solved[k]


def gather_columns(field, p, n, gathered):
    _, levels, ct, _ = field.shape
    lane_group = lax.broadcasted_iota(jnp.int32, (ct, 128), 1) // 4
    for k in range(levels):
        group = n * levels + k
        turned = pltpu.roll(field[p, k].astype(jnp.float32), (group * 4 + DEPTH) % 128, 1)
        gathered = jnp.where(lane_group == group, turned, gathered)
    return gathered


def columns_of(field, parity, half):
    gathered = jnp.zeros((field.shape[2], 128), jnp.float32)
    for n in range(half):
        gathered = gather_columns(field, 2 * n + parity, n, gathered)
    return gathered.T


def packed_columns(upright, group):
    pair = upright[(group // 2) * 8:(group // 2) * 8 + 8]
    return pltpu.roll(pair, 2 if group % 2 == 0 else 6, 0)


def packed_rows(field, p, k, low):
    ct = field.shape[2]
    top = field[p, k, 0:16].astype(jnp.float32)[0:8]
    bottom = field[p, k, ct - 16:ct].astype(jnp.float32)[8:16]
    return jnp.where(low, top, bottom)


def exchange_kernel(total, across, table_in, tracer, east_in, north_in, coupling_in, u, cols, rows,
                    table, q, east, north, coupling, s, r, d, h, own, drive, carry, ratio, still, ghost, change,
                    t_sem, q_sem, c_sem, send1, r_sem, send2, h_sem, peer, ready):
    panels, levels, ct, _ = q.shape
    half = panels // 2
    per = DEPTH * levels // HUBS
    first_hub = total // 2 - HUBS + 1
    me = lax.axis_index("tile")
    steps = (total - 1, across, 1, total - across)
    offsets = sorted(set(steps))

    def hub_flag(device):
        ahead = device - first_hub
        inside = jnp.logical_and(ahead >= 0, ahead < 2 * HUBS)
        return jnp.where(jnp.logical_and(inside, lax.rem(ahead + total, 2) == 0), 1, 0)

    am_hub = hub_flag(me)

    def load(p):
        return pltpu.make_async_copy(tracer.at[p], q.at[p], q_sem.at[p])

    fields = ((east_in, east), (north_in, north), (coupling_in, coupling))

    def loads(p):
        return [pltpu.make_async_copy(src.at[p], dst.at[p], c_sem.at[i, p]) for i, (src, dst) in enumerate(fields)]

    for parity in range(2):
        for n in range(half):
            load(2 * n + parity).start()
    fetch = pltpu.make_async_copy(table_in, table, t_sem)
    fetch.start()

    barrier = pltpu.get_barrier_semaphore()

    def signal(semaphore, device):
        pl.semaphore_signal(semaphore, inc=1, device_id={"tile": device}, device_id_type=pl.DeviceIdType.MESH)

    @pl.when(am_hub == 1)
    def _():
        def greet(i, carry):
            signal(barrier, lax.rem(me + i, total))
            return carry

        lax.fori_loop(1, total, greet, 0)

    @pl.when(am_hub == 0)
    def _():
        for offset in offsets:
            other = lax.rem(me + offset, total)

            @pl.when(other > me)
            def _():
                signal(barrier, other)

    expected, peers = HUBS - am_hub, 0
    for offset in offsets:
        other = lax.rem(me + offset, total)
        plain = 1 - hub_flag(other)
        expected = expected + jnp.where(other < me, plain, 0)
        peers = peers + jnp.where(other > me, plain, 0)

    def remote(src, dst, send, recv, device):
        return pltpu.make_async_remote_copy(
            src_ref=src, dst_ref=dst, send_sem=send, recv_sem=recv,
            device_id={"tile": device}, device_id_type=pl.DeviceIdType.MESH)

    flat = q.reshape(panels * levels * ct, 128)
    blocks = levels // per
    for parity in range(2):
        gathered = jnp.zeros((ct, 128), jnp.float32)
        for n in range(half):
            p = 2 * n + parity
            load(p).wait()
            gathered = gather_columns(q, p, n, gathered)
            for block in range(blocks):
                for depth in range(DEPTH):
                    x, base = depth * blocks + block, (p * levels + block * per) * ct
                    s[parity, 3, n, x] = flat[pl.ds(base + depth, per, stride=ct)]
                    s[parity, 1, n, x] = flat[pl.ds(base + ct - 1 - depth, per, stride=ct)]
        own[parity] = gathered.T
        for n in range(half):
            for block in range(blocks):
                base = (n * levels + block * per) * 4
                for c, (e, depth) in enumerate(((2, 1), (2, 0), (0, 0), (0, 1))):
                    s[parity, e, n, depth * blocks + block] = own[parity, pl.ds(base + c, per, stride=4)]
        if parity == 0:
            for n in range(half):
                for copy in loads(n):
                    copy.start()
            pl.semaphore_wait(barrier, expected)
        on, along = edge_state(me, parity, total, across)
        for e in range(4):
            @pl.when(on[e])
            def _():
                slot = ((parity * 4 + e) * across + along[e]) * half

                def spread(i, carry):
                    hub = first_hub + 2 * i
                    src, dst = s.at[parity, e, :, i], r.at[pl.ds(slot, half)]

                    @pl.when(hub != me)
                    def _():
                        remote(src, dst, send1.at[parity, e], r_sem, hub).start()

                    @pl.when(hub == me)
                    def _():
                        pltpu.make_async_copy(src, dst, r_sem).start()

                    return carry

                lax.fori_loop(0, HUBS, spread, 0)

    for n in range(half, panels):
        for copy in loads(n):
            copy.start()

    @pl.when(am_hub == 0)
    def _():
        for offset in offsets:
            other = lax.rem(me + offset, total)

            @pl.when(other < me)
            def _():
                signal(peer, other)

    for i in range(HUBS):
        @pl.when(me != first_hub + 2 * i)
        def _():
            signal(ready, first_hub + 2 * i)

    @pl.when(peers > 0)
    def _():
        pl.semaphore_wait(peer, peers)

    for parity in range(2):
        on, _ = edge_state(me, parity, total, across)
        for e in range(4):
            @pl.when(jnp.logical_not(on[e]))
            def _():
                far = (e + 2) % 4
                remote(s.at[parity, e], h.at[parity, far], send1.at[parity, e],
                       h_sem.at[parity, far], lax.rem(me + steps[e], total)).start()

    def compute(first, last):
        def one(p, carry):
            for copy in loads(p):
                copy.wait()
            update_panel(q, east, north, coupling, u, p)
            return carry

        lax.fori_loop(first, last, one, 0)

    compute(0, half)
    fetch.wait()

    @pl.when(am_hub == 1)
    def _():
        pl.semaphore_wait(ready, total - 1)
        pltpu.make_async_copy(r, r, r_sem).wait()
        seams = [(edge_tile(e, spot, across) + parity * (total // 2 + 1), parity, e, spot)
                 for parity in range(2) for e in range(4) for spot in range(across)]
        for owner, parity, e, spot in sorted((tile % total, *rest) for tile, *rest in seams):
            slot = ((parity * 4 + e) * across + spot) * half
            for n in range(half):
                p = 2 * n + parity
                other, f, turn = table[0, e, p], table[1, e, p], table[2, e, p]
                base = (lax.rem(other, 2) * 4 + f) * across * half + other // 2
                place = jnp.where(turn == 1, across - 1 - spot, spot)
                d[slot + n] = r[base + place * half]
            src = d.at[pl.ds(slot, half)]
            dst = h.at[parity, e, :, (me - first_hub) // 2]

            @pl.when(me != owner)
            def _():
                remote(src, dst, send2.at[parity, e], h_sem.at[parity, e], owner).start()

            @pl.when(me == owner)
            def _():
                pltpu.make_async_copy(src, dst, h_sem.at[parity, e]).start()

    compute(half, panels)

    sub = lax.broadcasted_iota(jnp.int32, (8, 128), 0)
    low, inner = sub < 4, jnp.logical_and(sub >= 2, sub < 6)
    for parity in range(2):
        north_columns = columns_of(north, parity, half)
        coupling_columns = columns_of(coupling, parity, half)
        for n in range(half):
            p = 2 * n + parity
            inverses, ratios = factors(
                lambda k: jnp.where(inner, packed_columns(coupling_columns, n * levels + k),
                                    packed_rows(coupling, p, k, low)), levels)
            for k in range(levels):
                group = n * levels + k
                coef = jnp.where(inner, packed_columns(north_columns, group), packed_rows(east, p, k, low))
                scaled = coef * inverses[k] * (-1.0 / 12.0)
                mine = packed_columns(own[parity, (group // 2) * 8:(group // 2) * 8 + 8], group % 2)
                back1, back2 = pltpu.roll(mine, 7, 0), pltpu.roll(mine, 6, 0)
                fore1, fore2 = pltpu.roll(mine, 1, 0), pltpu.roll(mine, 2, 0)
                part = jnp.where(sub == 2, back2, jnp.where(sub == 3, back2 - 8.0 * back1,
                                 jnp.where(sub == 4, 8.0 * fore1 - fore2, -fore2)))
                spot = parity * half * levels + group
                drive[spot] = scaled
                still[spot] = jnp.where(inner, part * scaled, 0.0)
                ratio[spot] = ratios[k]
                if k > 0:
                    carry[spot] = inverses[k] * below
                below = jnp.where(inner, packed_columns(coupling_columns, group), packed_rows(coupling, p, k, low))

    lane = lax.broadcasted_iota(jnp.int32, (levels, 128), 1)
    change[...] = jnp.zeros_like(change)
    for parity in range(2):
        on, _ = edge_state(me, parity, total, across)
        for e in range(4):
            pltpu.make_async_copy(h.at[parity, e], h.at[parity, e], h_sem.at[parity, e]).wait()
        for n in range(half):
            p = 2 * n + parity
            first = (parity * half + n) * levels * 8

            def ghosts(e):
                turned = jnp.logical_and(on[e], table[2, e, p] == 1)
                found = []
                for depth in range(DEPTH):
                    rows_in = jnp.concatenate([h[parity, e, n, depth * blocks + block] for block in range(blocks)], axis=0)
                    found.append(jnp.where(turned, jnp.take_along_axis(rows_in, 127 - lane, axis=1), rows_in))
                return found

            south, east_side, north_side, west = (ghosts(e) for e in range(4))
            for spots, (above1, above2), (below1, below2) in (
                    ((2, 3, 4, 5), north_side, south), ((6, 7, 0, 1), east_side, west)):
                values = (-above1, 8.0 * above1 - above2, below2 - 8.0 * below1, below1)
                for spot, value in zip(spots, values):
                    ghost[pl.ds(first + spot, levels, stride=8)] = value
        for n in range(half):
            start = (parity * half + n) * levels
            partials = []
            for k in range(levels):
                at = start + k
                current = ghost[at * 8:at * 8 + 8] * drive[at] + still[at]
                if k > 0:
                    current = current + carry[at] * partials[-1]
                partials.append(current)
            solved = [partials[-1]]
            for k in range(levels - 2, -1, -1):
                solved.insert(0, partials[k] + ratio[start + k] * solved[0])
            for k in range(levels):
                rows[start + k] = solved[k]
            for k in range(0, levels, 2):
                both = jnp.where(low, pltpu.roll(solved[k], 6, 0), pltpu.roll(solved[k + 1], 2, 0))
                change[parity, (n * levels + k) * 4:(n * levels + k) * 4 + 8] = both
        cols[parity] = change[parity].T

    def drain(ref, sem):
        pltpu.make_async_copy(ref, ref, sem).wait()

    for parity in range(2):
        on, _ = edge_state(me, parity, total, across)
        for e in range(4):
            base = (parity * 4 + e) * across * half
            seam_hub = jnp.logical_and(on[e], am_hub == 1)

            @pl.when(seam_hub)
            def _():
                drain(s.at[parity, e, :, pl.ds(0, HUBS - 1)], send1.at[parity, e])
                drain(d.at[pl.ds(base, (across - 1) * half)], send2.at[parity, e])

            @pl.when(jnp.logical_not(seam_hub))
            def _():
                drain(s.at[parity, e], send1.at[parity, e])

            @pl.when(jnp.logical_and(jnp.logical_not(on[e]), am_hub == 1))
            def _():
                drain(d.at[pl.ds(base, across * half)], send2.at[parity, e])


def finish_kernel(u, cols, rows, result, out, out_sem):
    panels, levels, ct, _ = u.shape
    half = panels // 2
    size = 8
    wide = lax.broadcasted_iota(jnp.int32, (size, 128), 1)
    sub = lax.broadcasted_iota(jnp.int32, (size, 128), 0)
    edge = jnp.logical_or(wide < DEPTH, wide >= 128 - DEPTH)
    for p in range(panels):
        n, parity = p // 2, p % 2
        for k in range(levels):
            group = n * levels + k
            extra = rows[parity * half * levels + group]
            for start in range(0, ct, size):
                patch = pltpu.roll(cols[parity, start:start + size], (126 - 4 * group) % 128, 1)
                value = u[p, k, start:start + size] + jnp.where(edge, patch, 0.0)
                if start == 0:
                    value = value + jnp.where(sub < DEPTH, extra, 0.0)
                if start == ct - size:
                    value = value + jnp.where(sub >= size - DEPTH, extra, 0.0)
                out[p, k, start:start + size] = value
        pltpu.make_async_copy(out.at[p], result.at[p], out_sem.at[p]).start()
    for p in range(panels):
        pltpu.make_async_copy(out.at[p], result.at[p], out_sem.at[p]).wait()


def solution(mesh):
    total = mesh.shape["tile"]
    across = math.isqrt(total)

    def shards(tracer, courant_east, courant_north, diffusivity, seam_table):
        _, panels, levels, ct, _ = tracer.shape
        half, per = panels // 2, DEPTH * levels // HUBS
        strips = (2, 4, half, HUBS, per, ct)
        units = (2 * 4 * across * half, per, ct)
        packs = (panels * levels, 8, ct)
        shape = tracer.shape[1:]
        anywhere = pl.BlockSpec(memory_space=pl.ANY)
        hbm = pl.BlockSpec(memory_space=pltpu.HBM)
        whole = pl.BlockSpec(memory_space=pltpu.VMEM)
        table = jnp.transpose(seam_table, (2, 1, 0))
        plain, cols, rows = pl.pallas_call(
            functools.partial(exchange_kernel, total, across),
            out_shape=[pltpu.VMEM(dims, jnp.float32) for dims in (shape, (2, ct, ct), packs)],
            in_specs=[hbm] * 5,
            out_specs=[whole] * 3,
            scratch_shapes=[
                pltpu.SMEM(table.shape, jnp.int32),
                pltpu.VMEM(shape, jnp.float32),
                pltpu.VMEM(shape, jnp.bfloat16),
                pltpu.VMEM(shape, jnp.bfloat16),
                pltpu.VMEM(shape, jnp.bfloat16),
                pltpu.VMEM(strips, jnp.float32),
                pltpu.VMEM(units, jnp.float32),
                pltpu.VMEM(units, jnp.float32),
                pltpu.VMEM(strips, jnp.float32),
                pltpu.VMEM((2, ct, ct), jnp.float32),
                pltpu.VMEM(packs, jnp.float32),
                pltpu.VMEM(packs, jnp.float32),
                pltpu.VMEM(packs, jnp.float32),
                pltpu.VMEM(packs, jnp.float32),
                pltpu.VMEM((panels * levels * 8, ct), jnp.float32),
                pltpu.VMEM((2, ct, ct), jnp.float32),
                pltpu.SemaphoreType.DMA,
                pltpu.SemaphoreType.DMA((panels,)),
                pltpu.SemaphoreType.DMA((3, panels)),
                pltpu.SemaphoreType.DMA((2, 4)),
                pltpu.SemaphoreType.DMA,
                pltpu.SemaphoreType.DMA((2, 4)),
                pltpu.SemaphoreType.DMA((2, 4)),
                pltpu.SemaphoreType.REGULAR,
                pltpu.SemaphoreType.REGULAR,
            ],
            compiler_params=pltpu.CompilerParams(collective_id=0, has_side_effects=True,
                                                 vmem_limit_bytes=VMEM_LIMIT),
            name="exchange",
        )(table, tracer[0], courant_east[0], courant_north[0], diffusivity[0])
        updated = pl.pallas_call(
            finish_kernel,
            out_shape=jax.ShapeDtypeStruct(shape, jnp.float32),
            in_specs=[whole] * 3,
            out_specs=anywhere,
            scratch_shapes=[pltpu.VMEM(shape, jnp.float32), pltpu.SemaphoreType.DMA((panels,))],
            compiler_params=pltpu.CompilerParams(vmem_limit_bytes=VMEM_LIMIT // 2),
            name="finish",
        )(plain, cols, rows)
        return updated[None]

    placed = P(("groups", "tile"), None, None, None, None)
    return jax.shard_map(
        shards, mesh=mesh, in_specs=(placed, placed, placed, placed, P()), out_specs=placed,
        check_vma=False)
```

```python
import functools
import math

import jax
import jax.numpy as jnp
from jax import lax
from jax.experimental import pallas as pl
from jax.experimental.pallas import tpu as pltpu
from jax.sharding import PartitionSpec as P

DEPTH = 2
HUBS = 4
LEVELS_AT_ONCE = 2
VMEM_LIMIT = 59 * 1024 * 1024


def tile_of(device, parity, total):
    return lax.rem(device + total - parity * (total // 2 + 1) + total, total)


def edge_state(device, parity, total, across):
    tile = tile_of(device, parity, total)
    row, col = tile // across, lax.rem(tile, across)
    on = (col == 0, row == across - 1, col == across - 1, row == 0)
    return on, (row, col, row, col)


def hubs_of(total, across):
    middle = total // 2
    return (middle - across + 1, middle - across + 3, middle + 1, middle + 3)


def edge_tile(edge, spot, across):
    return (spot * across, (across - 1) * across + spot, spot * across + across - 1, spot)[edge]


def central(q, p, k, start, size):
    ct = q.shape[2]
    mid = q[p, k, start:start + size]
    none = jnp.zeros((DEPTH, 128), jnp.float32)
    if start == 0:
        ext = jnp.concatenate([none, q[p, k, 0:size + DEPTH]], axis=0)
        near = [ext[o:o + size] for o in (0, 1, 3, 4)]
    elif start + size == ct:
        ext = jnp.concatenate([q[p, k, start - DEPTH:ct], none], axis=0)
        near = [ext[o:o + size] for o in (0, 1, 3, 4)]
    else:
        near = [q[p, k, start + o:start + o + size] for o in (-2, -1, 1, 2)]
    along_i = 8.0 * (near[2] - near[1]) - (near[3] - near[0])
    along_j = 8.0 * (pltpu.roll(mid, 127, 1) - pltpu.roll(mid, 1, 1)) - (
        pltpu.roll(mid, 126, 1) - pltpu.roll(mid, 2, 1))
    return mid, along_i, along_j


def factors(coupling, levels):
    inverses, ratios, below = [], [], None
    for k in range(levels):
        here = coupling(k)
        if k == 0:
            inverse = 1.0 / (1.0 + here)
        else:
            inverse = 1.0 / ((1.0 + here) + below * (1.0 - ratios[-1]))
        inverses.append(inverse)
        ratios.append(here * inverse)
        below = here
    return inverses, ratios


def solve(forced, coupling, levels):
    ratios, partials = [], []
    for k in range(levels):
        value, here = forced(k), coupling(k)
        if k == 0:
            inverse = 1.0 / (1.0 + here)
            current = value * inverse
        else:
            inverse = 1.0 / ((1.0 + here) + below * (1.0 - ratios[-1]))
            current = (value + below * partials[-1]) * inverse
        ratios.append(here * inverse)
        partials.append(current)
        below = here
    solved = [partials[-1]]
    for k in range(levels - 2, -1, -1):
        solved.insert(0, partials[k] + ratios[k] * solved[0])
    return solved


def update_panel(q, east, north, coupling, u, p):
    _, levels, ct, _ = q.shape
    size = 16
    for start in range(0, ct, size):
        part = pl.ds(start, size)

        def forced(k):
            mid, along_i, along_j = central(q, p, k, start, size)
            return mid - (east[p, k, part].astype(jnp.float32) * along_i
                          + north[p, k, part].astype(jnp.float32) * along_j) * (1.0 / 12.0)

        solved = solve(forced, lambda k: coupling[p, k, part].astype(jnp.float32), levels)
        for k in range(levels):
            u[p, k, part] = solved[k]


def gather_columns(field, p, n, gathered):
    _, levels, ct, _ = field.shape
    lane_group = lax.broadcasted_iota(jnp.int32, (ct, 128), 1) // 4
    for k in range(levels):
        group = n * levels + k
        turned = pltpu.roll(field[p, k].astype(jnp.float32), (group * 4 + DEPTH) % 128, 1)
        gathered = jnp.where(lane_group == group, turned, gathered)
    return gathered


def columns_of(field, parity, half):
    gathered = jnp.zeros((field.shape[2], 128), jnp.float32)
    for n in range(half):
        gathered = gather_columns(field, 2 * n + parity, n, gathered)
    return gathered.T


def packed_columns(upright, group):
    pair = upright[(group // 2) * 8:(group // 2) * 8 + 8]
    return pltpu.roll(pair, 2 if group % 2 == 0 else 6, 0)


def packed_rows(field, p, k, low):
    ct = field.shape[2]
    top = field[p, k, 0:16].astype(jnp.float32)[0:8]
    bottom = field[p, k, ct - 16:ct].astype(jnp.float32)[8:16]
    return jnp.where(low, top, bottom)


def exchange_kernel(total, across, table_in, tracer, east_in, north_in, coupling_in, u, cols, rows,
                    table, route, q, east, north, coupling, s, r, d, h, own, drive, carry, ratio, still, ghost, change,
                    t_sem, q_sem, c_sem, send1, r_sem, send2, h_sem, peer, ready):
    panels, levels, ct, _ = q.shape
    half = panels // 2
    per = DEPTH * levels // HUBS
    hubs = hubs_of(total, across)
    me = lax.axis_index("tile")
    steps = (total - 1, across, 1, total - across)
    offsets = sorted(set(steps))

    def hub_flag(device):
        flag = jnp.where(device == hubs[0], 1, 0)
        for hub in hubs[1:]:
            flag = flag + jnp.where(device == hub, 1, 0)
        return flag

    def hub_at(i):
        hub = hubs[0]
        for j in range(1, HUBS):
            hub = jnp.where(i == j, hubs[j], hub)
        return hub

    am_hub = hub_flag(me)

    def load(p):
        return pltpu.make_async_copy(tracer.at[p], q.at[p], q_sem.at[p])

    fields = ((east_in, east), (north_in, north), (coupling_in, coupling))

    def loads(p):
        return [pltpu.make_async_copy(src.at[p], dst.at[p], c_sem.at[i, p]) for i, (src, dst) in enumerate(fields)]

    for parity in range(2):
        for n in range(half):
            load(2 * n + parity).start()
    fetch = pltpu.make_async_copy(table_in, table, t_sem)
    fetch.start()

    barrier = pltpu.get_barrier_semaphore()

    def signal(semaphore, device):
        pl.semaphore_signal(semaphore, inc=1, device_id={"tile": device}, device_id_type=pl.DeviceIdType.MESH)

    @pl.when(am_hub == 1)
    def _():
        def greet(i, carry):
            signal(barrier, lax.rem(me + i, total))
            return carry

        lax.fori_loop(1, total, greet, 0)

    @pl.when(am_hub == 0)
    def _():
        for offset in offsets:
            other = lax.rem(me + offset, total)

            @pl.when(other > me)
            def _():
                signal(barrier, other)

    expected, peers = HUBS - am_hub, 0
    for offset in offsets:
        other = lax.rem(me + offset, total)
        plain = 1 - hub_flag(other)
        expected = expected + jnp.where(other < me, plain, 0)
        peers = peers + jnp.where(other > me, plain, 0)

    def remote(src, dst, send, recv, device):
        return pltpu.make_async_remote_copy(
            src_ref=src, dst_ref=dst, send_sem=send, recv_sem=recv,
            device_id={"tile": device}, device_id_type=pl.DeviceIdType.MESH)

    flat = q.reshape(panels * levels * ct, 128)
    blocks = levels // per
    early = me < across
    late = jnp.logical_not(early)
    deferred = jnp.logical_or(early, am_hub == 1)

    def prepare_rows(parity, n):
        p = 2 * n + parity
        for block in range(blocks):
            for depth in range(DEPTH):
                x, base = depth * blocks + block, (p * levels + block * per) * ct
                s[parity, 3, n, x] = flat[pl.ds(base + depth, per, stride=ct)]
                s[parity, 1, n, x] = flat[pl.ds(base + ct - 1 - depth, per, stride=ct)]

    def finish_columns(parity, gathered):
        own[parity] = gathered.T
        for n in range(half):
            for block in range(blocks):
                base = (n * levels + block * per) * 4
                for c, (e, depth) in enumerate(((2, 1), (2, 0), (0, 0), (0, 1))):
                    s[parity, e, n, depth * blocks + block] = own[parity, pl.ds(base + c, per, stride=4)]

    def enter():
        pl.semaphore_wait(barrier, expected)

        @pl.when(am_hub == 0)
        def _():
            for offset in offsets:
                other = lax.rem(me + offset, total)

                @pl.when(other < me)
                def _():
                    signal(peer, other)

        for hub in hubs:
            @pl.when(me != hub)
            def _():
                signal(ready, hub)

    def send_seams(parity, edges):
        on, along = edge_state(me, parity, total, across)
        for e in edges:
            @pl.when(on[e])
            def _():
                slot = ((parity * 4 + e) * across + along[e]) * half

                def spread(step, carry):
                    i = jnp.where(me * 2 < total, HUBS - 1 - step, step)
                    hub = hub_at(i)
                    src, dst = s.at[parity, e, :, i], r.at[pl.ds(slot, half)]

                    @pl.when(hub != me)
                    def _():
                        remote(src, dst, send1.at[parity, e], r_sem, hub).start()

                    @pl.when(hub == me)
                    def _():
                        pltpu.make_async_copy(src, dst, r_sem).start()

                    return carry

                lax.fori_loop(0, HUBS, spread, 0)

    def send_neighbours():
        @pl.when(peers > 0)
        def _():
            pl.semaphore_wait(peer, peers)

        for parity in range(2):
            on, _ = edge_state(me, parity, total, across)
            for e in range(4):
                @pl.when(jnp.logical_not(on[e]))
                def _():
                    far = (e + 2) % 4
                    remote(s.at[parity, e], h.at[parity, far], send1.at[parity, e],
                           h_sem.at[parity, far], lax.rem(me + steps[e], total)).start()

    for parity in range(2):
        gathered = jnp.zeros((ct, 128), jnp.float32)
        for n in range(half):
            load(2 * n + parity).wait()
            prepare_rows(parity, n)
            if n == 0 and parity == 0:
                gathered = gather_columns(q, parity, n, gathered)
        for n in (range(half) if parity == 0 else range(half, panels)):
            for copy in loads(n):
                copy.start()

        @pl.when(late)
        def _():
            if parity == 0:
                enter()
            send_seams(parity, (1, 3))

        for n in range(1 - parity, half):
            gathered = gather_columns(q, 2 * n + parity, n, gathered)
        finish_columns(parity, gathered)

        @pl.when(late)
        def _():
            send_seams(parity, (0, 2))

    @pl.when(early)
    def _():
        enter()
        for parity in range(2):
            send_seams(parity, range(4))

    @pl.when(jnp.logical_not(deferred))
    def _():
        send_neighbours()

    def arrive(which):
        for p in which:
            for copy in loads(p):
                copy.wait()

    def compute(first, last):
        def one(p, carry):
            update_panel(q, east, north, coupling, u, p)
            return carry

        lax.fori_loop(first, last, one, 0)

    fetch.wait()
    seams = [(edge_tile(e, spot, across) + parity * (total // 2 + 1), parity, e, spot)
             for parity in range(2) for e in range(4) for spot in range(across)]
    seams = sorted((tile % total, *rest) for tile, *rest in seams)

    @pl.when(am_hub == 1)
    def _():
        for e in range(4):
            for p in range(panels):
                other, f, turn = table[0, e, p], table[1, e, p], table[2, e, p]
                base = (lax.rem(other, 2) * 4 + f) * across * half + other // 2
                base = jnp.where(turn == 1, base + (across - 1) * half, base)
                step = jnp.where(turn == 1, -half, half)
                for spot in range(across):
                    route[((p % 2 * 4 + e) * across + spot) * half + p // 2] = base + step * spot

    arrive(range(half))
    compute(0, half)

    @pl.when(deferred)
    def _():
        send_neighbours()

    @pl.when(am_hub == 1)
    def _():
        pl.semaphore_wait(ready, total - 1)
        pltpu.make_async_copy(r, r, r_sem).wait()
        place = jnp.where(me == hubs[1], 1, 0) + jnp.where(me == hubs[2], 2, 0) + jnp.where(me == hubs[3], 3, 0)
        for owner, parity, e, spot in seams:
            slot = ((parity * 4 + e) * across + spot) * half
            for n in range(half):
                d[slot + n] = r[route[slot + n]]
            src = d.at[pl.ds(slot, half)]
            dst = h.at[parity, e, :, place]
            if owner in hubs:
                @pl.when(me != owner)
                def _():
                    remote(src, dst, send2.at[parity, e], h_sem.at[parity, e], owner).start()

                @pl.when(me == owner)
                def _():
                    pltpu.make_async_copy(src, dst, h_sem.at[parity, e]).start()
            else:
                remote(src, dst, send2.at[parity, e], h_sem.at[parity, e], owner).start()

    arrive(range(half, panels))
    sub = lax.broadcasted_iota(jnp.int32, (8, 128), 0)
    low, inner = sub < 4, jnp.logical_and(sub >= 2, sub < 6)
    for parity in range(2):
        north_columns = columns_of(north, parity, half)
        coupling_columns = columns_of(coupling, parity, half)
        for n in range(half):
            p = 2 * n + parity
            inverses, ratios = factors(
                lambda k: jnp.where(inner, packed_columns(coupling_columns, n * levels + k),
                                    packed_rows(coupling, p, k, low)), levels)
            for k in range(levels):
                group = n * levels + k
                coef = jnp.where(inner, packed_columns(north_columns, group), packed_rows(east, p, k, low))
                scaled = coef * inverses[k] * (-1.0 / 12.0)
                mine = packed_columns(own[parity, (group // 2) * 8:(group // 2) * 8 + 8], group % 2)
                back1, back2 = pltpu.roll(mine, 7, 0), pltpu.roll(mine, 6, 0)
                fore1, fore2 = pltpu.roll(mine, 1, 0), pltpu.roll(mine, 2, 0)
                part = jnp.where(sub == 2, back2, jnp.where(sub == 3, back2 - 8.0 * back1,
                                 jnp.where(sub == 4, 8.0 * fore1 - fore2, -fore2)))
                spot = parity * half * levels + group
                drive[spot] = scaled
                still[spot] = jnp.where(inner, part * scaled, 0.0)
                ratio[spot] = ratios[k]
                if k > 0:
                    carry[spot] = inverses[k] * below
                below = jnp.where(inner, packed_columns(coupling_columns, group), packed_rows(coupling, p, k, low))

    compute(half, panels)

    def drain(ref, sem):
        pltpu.make_async_copy(ref, ref, sem).wait()

    for parity in range(2):
        on, _ = edge_state(me, parity, total, across)
        for e in range(4):
            base = (parity * 4 + e) * across * half
            seam_hub = jnp.logical_and(on[e], am_hub == 1)

            @pl.when(seam_hub)
            def _():
                drain(s.at[parity, e, :, pl.ds(0, HUBS - 1)], send1.at[parity, e])
                drain(d.at[pl.ds(base, (across - 1) * half)], send2.at[parity, e])

            @pl.when(jnp.logical_not(seam_hub))
            def _():
                drain(s.at[parity, e], send1.at[parity, e])

            @pl.when(jnp.logical_and(jnp.logical_not(on[e]), am_hub == 1))
            def _():
                drain(d.at[pl.ds(base, across * half)], send2.at[parity, e])

    lane = lax.broadcasted_iota(jnp.int32, (levels, 128), 1)
    change[...] = jnp.zeros_like(change)
    for parity in range(2):
        for e in range(4):
            drain(h.at[parity, e], h_sem.at[parity, e])
    for parity in range(2):
        on, _ = edge_state(me, parity, total, across)
        for n in range(half):
            p = 2 * n + parity
            first = (parity * half + n) * levels * 8

            def ghosts(e):
                turned = jnp.logical_and(on[e], table[2, e, p] == 1)
                found = []
                for depth in range(DEPTH):
                    rows_in = jnp.concatenate([h[parity, e, n, depth * blocks + block] for block in range(blocks)], axis=0)
                    found.append(jnp.where(turned, jnp.take_along_axis(rows_in, 127 - lane, axis=1), rows_in))
                return found

            south, east_side, north_side, west = (ghosts(e) for e in range(4))
            for spots, (above1, above2), (below1, below2) in (
                    ((2, 3, 4, 5), north_side, south), ((6, 7, 0, 1), east_side, west)):
                values = (-above1, 8.0 * above1 - above2, below2 - 8.0 * below1, below1)
                for spot, value in zip(spots, values):
                    ghost[pl.ds(first + spot, levels, stride=8)] = value
    for parity in range(2):
        for n in range(half):
            start = (parity * half + n) * levels
            partials = []
            for k in range(levels):
                at = start + k
                current = ghost[at * 8:at * 8 + 8] * drive[at] + still[at]
                if k > 0:
                    current = current + carry[at] * partials[-1]
                partials.append(current)
            solved = [partials[-1]]
            for k in range(levels - 2, -1, -1):
                solved.insert(0, partials[k] + ratio[start + k] * solved[0])
            for k in range(levels):
                rows[start + k] = solved[k]
            for k in range(0, levels, 2):
                both = jnp.where(low, pltpu.roll(solved[k], 6, 0), pltpu.roll(solved[k + 1], 2, 0))
                change[parity, (n * levels + k) * 4:(n * levels + k) * 4 + 8] = both
    for parity in range(2):
        cols[parity] = change[parity].T


def finish_kernel(u, cols, rows, result, out, out_sem):
    panels, levels, ct, _ = u.shape
    half = panels // 2
    size = 8
    wide = lax.broadcasted_iota(jnp.int32, (size, 128), 1)
    sub = lax.broadcasted_iota(jnp.int32, (size, 128), 0)
    edge = jnp.logical_or(wide < DEPTH, wide >= 128 - DEPTH)

    def store(p, block):
        part = pl.ds(block * LEVELS_AT_ONCE, LEVELS_AT_ONCE)
        return pltpu.make_async_copy(out.at[p, part], result.at[p, part], out_sem.at[p, block])

    for p in range(panels):
        n, parity = p // 2, p % 2
        for k in range(levels):
            group = n * levels + k
            extra = rows[parity * half * levels + group]
            for start in range(0, ct, size):
                patch = pltpu.roll(cols[parity, start:start + size], (126 - 4 * group) % 128, 1)
                value = u[p, k, start:start + size] + jnp.where(edge, patch, 0.0)
                if start == 0:
                    value = value + jnp.where(sub < DEPTH, extra, 0.0)
                if start == ct - size:
                    value = value + jnp.where(sub >= size - DEPTH, extra, 0.0)
                out[p, k, start:start + size] = value
            if k % LEVELS_AT_ONCE == LEVELS_AT_ONCE - 1:
                store(p, k // LEVELS_AT_ONCE).start()
    for p in range(panels):
        for block in range(levels // LEVELS_AT_ONCE):
            store(p, block).wait()


def solution(mesh):
    total = mesh.shape["tile"]
    across = math.isqrt(total)

    def shards(tracer, courant_east, courant_north, diffusivity, seam_table):
        _, panels, levels, ct, _ = tracer.shape
        half, per = panels // 2, DEPTH * levels // HUBS
        strips = (2, 4, half, HUBS, per, ct)
        units = (2 * 4 * across * half, per, ct)
        packs = (panels * levels, 8, ct)
        shape = tracer.shape[1:]
        anywhere = pl.BlockSpec(memory_space=pl.ANY)
        hbm = pl.BlockSpec(memory_space=pltpu.HBM)
        whole = pl.BlockSpec(memory_space=pltpu.VMEM)
        table = jnp.transpose(seam_table, (2, 1, 0))
        plain, cols, rows = pl.pallas_call(
            functools.partial(exchange_kernel, total, across),
            out_shape=[pltpu.VMEM(dims, jnp.float32) for dims in (shape, (2, ct, ct), packs)],
            in_specs=[hbm] * 5,
            out_specs=[whole] * 3,
            scratch_shapes=[
                pltpu.SMEM(table.shape, jnp.int32),
                pltpu.SMEM(units[:1], jnp.int32),
                pltpu.VMEM(shape, jnp.float32),
                pltpu.VMEM(shape, jnp.bfloat16),
                pltpu.VMEM(shape, jnp.bfloat16),
                pltpu.VMEM(shape, jnp.bfloat16),
                pltpu.VMEM(strips, jnp.float32),
                pltpu.VMEM(units, jnp.float32),
                pltpu.VMEM(units, jnp.float32),
                pltpu.VMEM(strips, jnp.float32),
                pltpu.VMEM((2, ct, ct), jnp.float32),
                pltpu.VMEM(packs, jnp.float32),
                pltpu.VMEM(packs, jnp.float32),
                pltpu.VMEM(packs, jnp.float32),
                pltpu.VMEM(packs, jnp.float32),
                pltpu.VMEM((panels * levels * 8, ct), jnp.float32),
                pltpu.VMEM((2, ct, ct), jnp.float32),
                pltpu.SemaphoreType.DMA,
                pltpu.SemaphoreType.DMA((panels,)),
                pltpu.SemaphoreType.DMA((3, panels)),
                pltpu.SemaphoreType.DMA((2, 4)),
                pltpu.SemaphoreType.DMA,
                pltpu.SemaphoreType.DMA((2, 4)),
                pltpu.SemaphoreType.DMA((2, 4)),
                pltpu.SemaphoreType.REGULAR,
                pltpu.SemaphoreType.REGULAR,
            ],
            compiler_params=pltpu.CompilerParams(collective_id=0, has_side_effects=True,
                                                 vmem_limit_bytes=VMEM_LIMIT),
            name="exchange",
        )(table, tracer[0], courant_east[0], courant_north[0], diffusivity[0])
        updated = pl.pallas_call(
            finish_kernel,
            out_shape=jax.ShapeDtypeStruct(shape, jnp.float32),
            in_specs=[whole] * 3,
            out_specs=anywhere,
            scratch_shapes=[pltpu.VMEM(shape, jnp.float32), pltpu.SemaphoreType.DMA((panels, levels // LEVELS_AT_ONCE))],
            compiler_params=pltpu.CompilerParams(vmem_limit_bytes=VMEM_LIMIT // 2),
            name="finish",
        )(plain, cols, rows)
        return updated[None]

    placed = P(("groups", "tile"), None, None, None, None)
    return jax.shard_map(
        shards, mesh=mesh, in_specs=(placed, placed, placed, placed, P()), out_specs=placed,
        check_vma=False)
```

```python
import functools
import math

import jax
import jax.numpy as jnp
from jax import lax
from jax.experimental import pallas as pl
from jax.experimental.pallas import tpu as pltpu
from jax.sharding import PartitionSpec as P

DEPTH = 2
HUBS = 4
LEVELS_AT_ONCE = 2
VMEM_LIMIT = 59 * 1024 * 1024


def tile_of(device, parity, total):
    return lax.rem(device + total - parity * (total // 2 + 1) + total, total)


def edge_state(device, parity, total, across):
    tile = tile_of(device, parity, total)
    row, col = tile // across, lax.rem(tile, across)
    on = (col == 0, row == across - 1, col == across - 1, row == 0)
    return on, (row, col, row, col)


def hubs_of(total, across):
    middle = total // 2
    return (middle - across, middle - across + 1, middle - across + 3, middle + 1)


def edge_tile(edge, spot, across):
    return (spot * across, (across - 1) * across + spot, spot * across + across - 1, spot)[edge]


def central(q, p, k, start, size):
    ct = q.shape[2]
    mid = q[p, k, start:start + size]
    none = jnp.zeros((DEPTH, 128), jnp.float32)
    if start == 0:
        ext = jnp.concatenate([none, q[p, k, 0:size + DEPTH]], axis=0)
        near = [ext[o:o + size] for o in (0, 1, 3, 4)]
    elif start + size == ct:
        ext = jnp.concatenate([q[p, k, start - DEPTH:ct], none], axis=0)
        near = [ext[o:o + size] for o in (0, 1, 3, 4)]
    else:
        near = [q[p, k, start + o:start + o + size] for o in (-2, -1, 1, 2)]
    along_i = 8.0 * (near[2] - near[1]) - (near[3] - near[0])
    along_j = 8.0 * (pltpu.roll(mid, 127, 1) - pltpu.roll(mid, 1, 1)) - (
        pltpu.roll(mid, 126, 1) - pltpu.roll(mid, 2, 1))
    return mid, along_i, along_j


def factors(coupling, levels):
    inverses, ratios, below = [], [], None
    for k in range(levels):
        here = coupling(k)
        if k == 0:
            inverse = 1.0 / (1.0 + here)
        else:
            inverse = 1.0 / ((1.0 + here) + below * (1.0 - ratios[-1]))
        inverses.append(inverse)
        ratios.append(here * inverse)
        below = here
    return inverses, ratios


def solve(forced, coupling, levels):
    ratios, partials = [], []
    for k in range(levels):
        value, here = forced(k), coupling(k)
        if k == 0:
            inverse = 1.0 / (1.0 + here)
            current = value * inverse
        else:
            inverse = 1.0 / ((1.0 + here) + below * (1.0 - ratios[-1]))
            current = (value + below * partials[-1]) * inverse
        ratios.append(here * inverse)
        partials.append(current)
        below = here
    solved = [partials[-1]]
    for k in range(levels - 2, -1, -1):
        solved.insert(0, partials[k] + ratios[k] * solved[0])
    return solved


def update_panel(q, east, north, coupling, u, p):
    _, levels, ct, _ = q.shape
    size = 16
    for start in range(0, ct, size):
        part = pl.ds(start, size)

        def forced(k):
            mid, along_i, along_j = central(q, p, k, start, size)
            return mid - (east[p, k, part].astype(jnp.float32) * along_i
                          + north[p, k, part].astype(jnp.float32) * along_j) * (1.0 / 12.0)

        solved = solve(forced, lambda k: coupling[p, k, part].astype(jnp.float32), levels)
        for k in range(levels):
            u[p, k, part] = solved[k]


def gather_columns(field, p, n, gathered):
    _, levels, ct, _ = field.shape
    lane_group = lax.broadcasted_iota(jnp.int32, (ct, 128), 1) // 4
    for k in range(levels):
        group = n * levels + k
        turned = pltpu.roll(field[p, k].astype(jnp.float32), (group * 4 + DEPTH) % 128, 1)
        gathered = jnp.where(lane_group == group, turned, gathered)
    return gathered


def columns_of(field, parity, half):
    gathered = jnp.zeros((field.shape[2], 128), jnp.float32)
    for n in range(half):
        gathered = gather_columns(field, 2 * n + parity, n, gathered)
    return gathered.T


def packed_columns(upright, group):
    pair = upright[(group // 2) * 8:(group // 2) * 8 + 8]
    return pltpu.roll(pair, 2 if group % 2 == 0 else 6, 0)


def packed_rows(field, p, k, low):
    ct = field.shape[2]
    top = field[p, k, 0:16].astype(jnp.float32)[0:8]
    bottom = field[p, k, ct - 16:ct].astype(jnp.float32)[8:16]
    return jnp.where(low, top, bottom)


def exchange_kernel(total, across, table_in, tracer, east_in, north_in, coupling_in, u, cols, rows,
                    table, route, q, fields, s, r, d, h, own, drive, carry, ratio, still, ghost, change,
                    t_sem, q_sem, c_sem, send1, r_sem, send2, h_sem, peer, ready):
    panels, levels, ct, _ = q.shape
    half = panels // 2
    per = DEPTH * levels // HUBS
    hubs = hubs_of(total, across)
    me = lax.axis_index("tile")
    steps = (total - 1, across, 1, total - across)
    offsets = sorted(set(steps))

    def hub_flag(device):
        flag = jnp.where(device == hubs[0], 1, 0)
        for hub in hubs[1:]:
            flag = flag + jnp.where(device == hub, 1, 0)
        return flag

    am_hub = hub_flag(me)

    def load(p, stage):
        pltpu.make_async_copy(tracer.at[p], q.at[p], q_sem.at[stage]).start()

    def drain(ref, sem):
        pltpu.make_async_copy(ref, ref, sem).wait()

    def load_fields(stage):
        part = pl.ds(stage * half, half)
        for i, src in enumerate((east_in, north_in, coupling_in)):
            pltpu.make_async_copy(src.at[part], fields.at[i, part], c_sem.at[stage]).start()

    def arrive(stage):
        drain(fields.at[:, pl.ds(stage * half, half)], c_sem.at[stage])

    east, north, coupling = (fields.at[i] for i in range(3))
    load(0, 0)
    for n in range(1, half):
        load(2 * n, 1)
    for n in range(half):
        load(2 * n + 1, 2)
    fetch = pltpu.make_async_copy(table_in, table, t_sem)
    fetch.start()

    barrier = pltpu.get_barrier_semaphore()

    def signal(semaphore, device):
        pl.semaphore_signal(semaphore, inc=1, device_id={"tile": device}, device_id_type=pl.DeviceIdType.MESH)

    @pl.when(am_hub == 1)
    def _():
        def greet(i, carry):
            signal(barrier, lax.rem(me + i, total))
            return carry

        lax.fori_loop(1, total, greet, 0)

    @pl.when(am_hub == 0)
    def _():
        for offset in offsets:
            other = lax.rem(me + offset, total)

            @pl.when(other > me)
            def _():
                signal(barrier, other)

    expected, peers = HUBS - am_hub, 0
    for offset in offsets:
        other = lax.rem(me + offset, total)
        plain = 1 - hub_flag(other)
        expected = expected + jnp.where(other < me, plain, 0)
        peers = peers + jnp.where(other > me, plain, 0)

    def remote(src, dst, send, recv, device):
        return pltpu.make_async_remote_copy(
            src_ref=src, dst_ref=dst, send_sem=send, recv_sem=recv,
            device_id={"tile": device}, device_id_type=pl.DeviceIdType.MESH)

    flat = q.reshape(panels * levels * ct, 128)
    blocks = levels // per
    early = me < across
    late = jnp.logical_not(early)
    deferred = jnp.logical_or(early, am_hub == 1)

    def prepare_rows(parity, n):
        p = 2 * n + parity
        for block in range(blocks):
            for depth in range(DEPTH):
                x, base = depth * blocks + block, (p * levels + block * per) * ct
                s[parity, 3, n, x] = flat[pl.ds(base + depth, per, stride=ct)]
                s[parity, 1, n, x] = flat[pl.ds(base + ct - 1 - depth, per, stride=ct)]

    def finish_columns(parity, gathered):
        own[parity] = gathered.T
        for n in range(half):
            for block in range(blocks):
                base = (n * levels + block * per) * 4
                for c, (e, depth) in enumerate(((2, 1), (2, 0), (0, 0), (0, 1))):
                    s[parity, e, n, depth * blocks + block] = own[parity, pl.ds(base + c, per, stride=4)]

    def tell():
        @pl.when(am_hub == 0)
        def _():
            for offset in offsets:
                other = lax.rem(me + offset, total)

                @pl.when(other < me)
                def _():
                    signal(peer, other)

        for hub in hubs:
            @pl.when(me != hub)
            def _():
                signal(ready, hub)

    def send_seams(parity, edges, order):
        on, along = edge_state(me, parity, total, across)
        for e in edges:
            @pl.when(on[e])
            def _():
                slot = ((parity * 4 + e) * across + along[e]) * half

                def piece(i):
                    return s.at[parity, e, :, i], r.at[pl.ds(slot, half)]

                @pl.when(am_hub == 0)
                def _():
                    for i in order:
                        src, dst = piece(i)
                        remote(src, dst, send1, r_sem, hubs[i]).start()

                @pl.when(am_hub == 1)
                def _():
                    for i in order:
                        src, dst = piece(i)

                        @pl.when(me != hubs[i])
                        def _():
                            remote(src, dst, send1, r_sem, hubs[i]).start()

                        @pl.when(me == hubs[i])
                        def _():
                            pltpu.make_async_copy(src, dst, r_sem).start()

    def send_neighbours():
        @pl.when(peers > 0)
        def _():
            pl.semaphore_wait(peer, peers)

        for parity in range(2):
            on, _ = edge_state(me, parity, total, across)
            for e in range(4):
                @pl.when(jnp.logical_not(on[e]))
                def _():
                    far = (e + 2) % 4
                    remote(s.at[parity, e], h.at[parity, far], send1, h_sem,
                           lax.rem(me + steps[e], total)).start()

    for parity in range(2):
        gathered = jnp.zeros((ct, 128), jnp.float32)
        if parity == 0:
            drain(q.at[0], q_sem.at[0])
            prepare_rows(0, 0)
            gathered = gather_columns(q, 0, 0, gathered)
            drain(q.at[pl.ds(0, half - 1)], q_sem.at[1])
        else:
            drain(q.at[pl.ds(0, half)], q_sem.at[2])
        for n in range(1 - parity, half):
            prepare_rows(parity, n)
        load_fields(parity)

        @pl.when(late)
        def _():
            if parity == 0:
                pl.semaphore_wait(barrier, expected)
            send_seams(parity, (1, 3), range(HUBS))
            if parity == 0:
                tell()

        for n in range(1 - parity, half):
            gathered = gather_columns(q, 2 * n + parity, n, gathered)
        finish_columns(parity, gathered)

        @pl.when(late)
        def _():
            send_seams(parity, (0, 2), range(HUBS))

    @pl.when(early)
    def _():
        pl.semaphore_wait(barrier, expected)
        for parity in range(2):
            send_seams(parity, range(4), range(HUBS - 1, -1, -1))
        tell()

    @pl.when(jnp.logical_not(deferred))
    def _():
        send_neighbours()

    def compute(first, last):
        def one(p, carry):
            update_panel(q, east, north, coupling, u, p)
            return carry

        lax.fori_loop(first, last, one, 0)

    fetch.wait()
    seams = [(edge_tile(e, spot, across) + parity * (total // 2 + 1), parity, e, spot)
             for parity in range(2) for e in range(4) for spot in range(across)]
    seams = sorted((tile % total, *rest) for tile, *rest in seams)

    @pl.when(am_hub == 1)
    def _():
        for e in range(4):
            for p in range(panels):
                other, f, turn = table[0, e, p], table[1, e, p], table[2, e, p]
                base = (lax.rem(other, 2) * 4 + f) * across * half + other // 2
                base = jnp.where(turn == 1, base + (across - 1) * half, base)
                step = jnp.where(turn == 1, -half, half)
                for spot in range(across):
                    route[((p % 2 * 4 + e) * across + spot) * half + p // 2] = base + step * spot

    arrive(0)
    compute(0, half)

    @pl.when(deferred)
    def _():
        send_neighbours()

    @pl.when(am_hub == 1)
    def _():
        pl.semaphore_wait(ready, total - 1)
        pltpu.make_async_copy(r, r, r_sem).wait()
        place = jnp.where(me == hubs[1], 1, 0) + jnp.where(me == hubs[2], 2, 0) + jnp.where(me == hubs[3], 3, 0)
        for owner, parity, e, spot in seams:
            slot = ((parity * 4 + e) * across + spot) * half
            for n in range(half):
                d[slot + n] = r[route[slot + n]]
            src = d.at[pl.ds(slot, half)]
            dst = h.at[parity, e, :, place]
            if owner in hubs:
                @pl.when(me != owner)
                def _():
                    remote(src, dst, send2, h_sem, owner).start()

                @pl.when(me == owner)
                def _():
                    pltpu.make_async_copy(src, dst, h_sem).start()
            else:
                remote(src, dst, send2, h_sem, owner).start()

    arrive(1)
    sub = lax.broadcasted_iota(jnp.int32, (8, 128), 0)
    low, inner = sub < 4, jnp.logical_and(sub >= 2, sub < 6)
    for parity in range(2):
        north_columns = columns_of(north, parity, half)
        coupling_columns = columns_of(coupling, parity, half)
        for n in range(half):
            p = 2 * n + parity
            inverses, ratios = factors(
                lambda k: jnp.where(inner, packed_columns(coupling_columns, n * levels + k),
                                    packed_rows(coupling, p, k, low)), levels)
            for k in range(levels):
                group = n * levels + k
                coef = jnp.where(inner, packed_columns(north_columns, group), packed_rows(east, p, k, low))
                scaled = coef * inverses[k] * (-1.0 / 12.0)
                mine = packed_columns(own[parity, (group // 2) * 8:(group // 2) * 8 + 8], group % 2)
                back1, back2 = pltpu.roll(mine, 7, 0), pltpu.roll(mine, 6, 0)
                fore1, fore2 = pltpu.roll(mine, 1, 0), pltpu.roll(mine, 2, 0)
                part = jnp.where(sub == 2, back2, jnp.where(sub == 3, back2 - 8.0 * back1,
                                 jnp.where(sub == 4, 8.0 * fore1 - fore2, -fore2)))
                spot = parity * half * levels + group
                drive[spot] = scaled
                still[spot] = jnp.where(inner, part * scaled, 0.0)
                ratio[spot] = ratios[k]
                if k > 0:
                    carry[spot] = inverses[k] * below
                below = jnp.where(inner, packed_columns(coupling_columns, group), packed_rows(coupling, p, k, low))

    compute(half, panels)

    seam_edges = 0
    for parity in range(2):
        on, _ = edge_state(me, parity, total, across)
        for e in range(4):
            seam_edges = seam_edges + jnp.where(on[e], 1, 0)
    for count in range(5):
        @pl.when(seam_edges * am_hub == count)
        def _():
            drain(r.at[pl.ds(0, (8 * HUBS - count) * half)], send1)

        @pl.when(jnp.logical_and(seam_edges == count, am_hub == 1))
        def _():
            drain(d.at[pl.ds(0, (8 * across - count) * half)], send2)

    lane = lax.broadcasted_iota(jnp.int32, (levels, 128), 1)
    change[...] = jnp.zeros_like(change)
    drain(h, h_sem)
    for parity in range(2):
        on, _ = edge_state(me, parity, total, across)
        for n in range(half):
            p = 2 * n + parity
            first = (parity * half + n) * levels * 8

            def ghosts(e):
                turned = jnp.logical_and(on[e], table[2, e, p] == 1)
                found = []
                for depth in range(DEPTH):
                    rows_in = jnp.concatenate([h[parity, e, n, depth * blocks + block] for block in range(blocks)], axis=0)
                    found.append(jnp.where(turned, jnp.take_along_axis(rows_in, 127 - lane, axis=1), rows_in))
                return found

            south, east_side, north_side, west = (ghosts(e) for e in range(4))
            for spots, (above1, above2), (below1, below2) in (
                    ((2, 3, 4, 5), north_side, south), ((6, 7, 0, 1), east_side, west)):
                values = (-above1, 8.0 * above1 - above2, below2 - 8.0 * below1, below1)
                for spot, value in zip(spots, values):
                    ghost[pl.ds(first + spot, levels, stride=8)] = value
    for parity in range(2):
        for n in range(half):
            start = (parity * half + n) * levels
            partials = []
            for k in range(levels):
                at = start + k
                current = ghost[at * 8:at * 8 + 8] * drive[at] + still[at]
                if k > 0:
                    current = current + carry[at] * partials[-1]
                partials.append(current)
            solved = [partials[-1]]
            for k in range(levels - 2, -1, -1):
                solved.insert(0, partials[k] + ratio[start + k] * solved[0])
            for k in range(levels):
                rows[start + k] = solved[k]
            for k in range(0, levels, 2):
                both = jnp.where(low, pltpu.roll(solved[k], 6, 0), pltpu.roll(solved[k + 1], 2, 0))
                change[parity, (n * levels + k) * 4:(n * levels + k) * 4 + 8] = both
    for parity in range(2):
        cols[parity] = change[parity].T


def finish_kernel(u, cols, rows, result, out, out_sem):
    panels, levels, ct, _ = u.shape
    half = panels // 2
    size = 8
    wide = lax.broadcasted_iota(jnp.int32, (size, 128), 1)
    sub = lax.broadcasted_iota(jnp.int32, (size, 128), 0)
    edge = jnp.logical_or(wide < DEPTH, wide >= 128 - DEPTH)

    def store(p, block):
        part = pl.ds(block * LEVELS_AT_ONCE, LEVELS_AT_ONCE)
        return pltpu.make_async_copy(out.at[p, part], result.at[p, part], out_sem)

    for p in range(panels):
        n, parity = p // 2, p % 2
        for k in range(levels):
            group = n * levels + k
            extra = rows[parity * half * levels + group]
            for start in range(0, ct, size):
                patch = pltpu.roll(cols[parity, start:start + size], (126 - 4 * group) % 128, 1)
                value = u[p, k, start:start + size] + jnp.where(edge, patch, 0.0)
                if start == 0:
                    value = value + jnp.where(sub < DEPTH, extra, 0.0)
                if start == ct - size:
                    value = value + jnp.where(sub >= size - DEPTH, extra, 0.0)
                out[p, k, start:start + size] = value
            if k % LEVELS_AT_ONCE == LEVELS_AT_ONCE - 1:
                store(p, k // LEVELS_AT_ONCE).start()
    pltpu.make_async_copy(out, result, out_sem).wait()


def solution(mesh):
    total = mesh.shape["tile"]
    across = math.isqrt(total)

    def shards(tracer, courant_east, courant_north, diffusivity, seam_table):
        _, panels, levels, ct, _ = tracer.shape
        half, per = panels // 2, DEPTH * levels // HUBS
        strips = (2, 4, half, HUBS, per, ct)
        units = (2 * 4 * across * half, per, ct)
        packs = (panels * levels, 8, ct)
        shape = tracer.shape[1:]
        anywhere = pl.BlockSpec(memory_space=pl.ANY)
        hbm = pl.BlockSpec(memory_space=pltpu.HBM)
        whole = pl.BlockSpec(memory_space=pltpu.VMEM)
        table = jnp.transpose(seam_table, (2, 1, 0))
        plain, cols, rows = pl.pallas_call(
            functools.partial(exchange_kernel, total, across),
            out_shape=[pltpu.VMEM(dims, jnp.float32) for dims in (shape, (2, ct, ct), packs)],
            in_specs=[hbm] * 5,
            out_specs=[whole] * 3,
            scratch_shapes=[
                pltpu.SMEM(table.shape, jnp.int32),
                pltpu.SMEM(units[:1], jnp.int32),
                pltpu.VMEM(shape, jnp.float32),
                pltpu.VMEM((3,) + shape, jnp.bfloat16),
                pltpu.VMEM(strips, jnp.float32),
                pltpu.VMEM(units, jnp.float32),
                pltpu.VMEM(units, jnp.float32),
                pltpu.VMEM(strips, jnp.float32),
                pltpu.VMEM((2, ct, ct), jnp.float32),
                pltpu.VMEM(packs, jnp.float32),
                pltpu.VMEM(packs, jnp.float32),
                pltpu.VMEM(packs, jnp.float32),
                pltpu.VMEM(packs, jnp.float32),
                pltpu.VMEM((panels * levels * 8, ct), jnp.float32),
                pltpu.VMEM((2, ct, ct), jnp.float32),
                pltpu.SemaphoreType.DMA,
                pltpu.SemaphoreType.DMA((3,)),
                pltpu.SemaphoreType.DMA((2,)),
                pltpu.SemaphoreType.DMA,
                pltpu.SemaphoreType.DMA,
                pltpu.SemaphoreType.DMA,
                pltpu.SemaphoreType.DMA,
                pltpu.SemaphoreType.REGULAR,
                pltpu.SemaphoreType.REGULAR,
            ],
            compiler_params=pltpu.CompilerParams(collective_id=0, has_side_effects=True,
                                                 vmem_limit_bytes=VMEM_LIMIT),
            name="exchange",
        )(table, tracer[0], courant_east[0], courant_north[0], diffusivity[0])
        updated = pl.pallas_call(
            finish_kernel,
            out_shape=jax.ShapeDtypeStruct(shape, jnp.float32),
            in_specs=[whole] * 3,
            out_specs=anywhere,
            scratch_shapes=[pltpu.VMEM(shape, jnp.float32), pltpu.SemaphoreType.DMA],
            compiler_params=pltpu.CompilerParams(vmem_limit_bytes=VMEM_LIMIT // 2),
            name="finish",
        )(plain, cols, rows)
        return updated[None]

    placed = P(("groups", "tile"), None, None, None, None)
    return jax.shard_map(
        shards, mesh=mesh, in_specs=(placed, placed, placed, placed, P()), out_specs=placed,
        check_vma=False)
```

```python
import functools
import math

import jax
import jax.numpy as jnp
from jax import lax
from jax.experimental import pallas as pl
from jax.experimental.pallas import tpu as pltpu
from jax.sharding import PartitionSpec as P

DEPTH = 2
HUBS = 4
LEVELS_AT_ONCE = 2
VMEM_LIMIT = 59 * 1024 * 1024


def tile_of(device, parity, total):
    return lax.rem(device + total - parity * (total // 2 + 1) + total, total)


def edge_state(device, parity, total, across):
    tile = tile_of(device, parity, total)
    row, col = tile // across, lax.rem(tile, across)
    on = (col == 0, row == across - 1, col == across - 1, row == 0)
    return on, (row, col, row, col)


def hubs_of(total, across):
    middle = total // 2
    return (middle - across - 1, middle - across + 1, middle - across + 3, middle + 1)


def edge_tile(edge, spot, across):
    return (spot * across, (across - 1) * across + spot, spot * across + across - 1, spot)[edge]


def central(q, p, k, start, size):
    ct = q.shape[2]
    mid = q[p, k, start:start + size]
    none = jnp.zeros((DEPTH, 128), jnp.float32)
    if start == 0:
        ext = jnp.concatenate([none, q[p, k, 0:size + DEPTH]], axis=0)
        near = [ext[o:o + size] for o in (0, 1, 3, 4)]
    elif start + size == ct:
        ext = jnp.concatenate([q[p, k, start - DEPTH:ct], none], axis=0)
        near = [ext[o:o + size] for o in (0, 1, 3, 4)]
    else:
        near = [q[p, k, start + o:start + o + size] for o in (-2, -1, 1, 2)]
    along_i = 8.0 * (near[2] - near[1]) - (near[3] - near[0])
    along_j = 8.0 * (pltpu.roll(mid, 127, 1) - pltpu.roll(mid, 1, 1)) - (
        pltpu.roll(mid, 126, 1) - pltpu.roll(mid, 2, 1))
    return mid, along_i, along_j


def factors(coupling, levels):
    inverses, ratios, below = [], [], None
    for k in range(levels):
        here = coupling(k)
        if k == 0:
            inverse = 1.0 / (1.0 + here)
        else:
            inverse = 1.0 / ((1.0 + here) + below * (1.0 - ratios[-1]))
        inverses.append(inverse)
        ratios.append(here * inverse)
        below = here
    return inverses, ratios


def solve(forced, coupling, levels):
    ratios, partials = [], []
    for k in range(levels):
        value, here = forced(k), coupling(k)
        if k == 0:
            inverse = 1.0 / (1.0 + here)
            current = value * inverse
        else:
            inverse = 1.0 / ((1.0 + here) + below * (1.0 - ratios[-1]))
            current = (value + below * partials[-1]) * inverse
        ratios.append(here * inverse)
        partials.append(current)
        below = here
    solved = [partials[-1]]
    for k in range(levels - 2, -1, -1):
        solved.insert(0, partials[k] + ratios[k] * solved[0])
    return solved


def update_panel(q, east, north, coupling, u, p):
    _, levels, ct, _ = q.shape
    size = 16
    for start in range(0, ct, size):
        part = pl.ds(start, size)

        def forced(k):
            mid, along_i, along_j = central(q, p, k, start, size)
            return mid - (east[p, k, part].astype(jnp.float32) * along_i
                          + north[p, k, part].astype(jnp.float32) * along_j) * (1.0 / 12.0)

        solved = solve(forced, lambda k: coupling[p, k, part].astype(jnp.float32), levels)
        for k in range(levels):
            u[p, k, part] = solved[k]


def gather_columns(field, p, n, gathered):
    _, levels, ct, _ = field.shape
    lane_group = lax.broadcasted_iota(jnp.int32, (ct, 128), 1) // 4
    for k in range(levels):
        group = n * levels + k
        turned = pltpu.roll(field[p, k].astype(jnp.float32), (group * 4 + DEPTH) % 128, 1)
        gathered = jnp.where(lane_group == group, turned, gathered)
    return gathered


def columns_of(field, parity, half):
    gathered = jnp.zeros((field.shape[2], 128), jnp.float32)
    for n in range(half):
        gathered = gather_columns(field, 2 * n + parity, n, gathered)
    return gathered.T


def packed_columns(upright, group):
    pair = upright[(group // 2) * 8:(group // 2) * 8 + 8]
    return pltpu.roll(pair, 2 if group % 2 == 0 else 6, 0)


def packed_rows(field, p, k, low):
    ct = field.shape[2]
    top = field[p, k, 0:16].astype(jnp.float32)[0:8]
    bottom = field[p, k, ct - 16:ct].astype(jnp.float32)[8:16]
    return jnp.where(low, top, bottom)


def exchange_kernel(total, across, table_in, tracer, east_in, north_in, coupling_in, u, cols, rows,
                    table, route, q, fields, s, r, d, h, own, drive, carry, ratio, still, ghost, change,
                    t_sem, q_sem, c_sem, send1, r_sem, send2, h_sem, peer, ready):
    panels, levels, ct, _ = q.shape
    half = panels // 2
    per = DEPTH * levels // HUBS
    hubs = hubs_of(total, across)
    me = lax.axis_index("tile")
    steps = (total - 1, across, 1, total - across)
    offsets = sorted(set(steps))

    def hub_flag(device):
        flag = jnp.where(device == hubs[0], 1, 0)
        for hub in hubs[1:]:
            flag = flag + jnp.where(device == hub, 1, 0)
        return flag

    am_hub = hub_flag(me)

    def load(p, stage):
        pltpu.make_async_copy(tracer.at[p], q.at[p], q_sem.at[stage]).start()

    def drain(ref, sem):
        pltpu.make_async_copy(ref, ref, sem).wait()

    def load_fields(stage):
        part = pl.ds(stage * half, half)
        for i, src in enumerate((east_in, north_in, coupling_in)):
            pltpu.make_async_copy(src.at[part], fields.at[i, part], c_sem.at[stage]).start()

    def arrive(stage):
        drain(fields.at[:, pl.ds(stage * half, half)], c_sem.at[stage])

    east, north, coupling = (fields.at[i] for i in range(3))
    load(0, 0)
    for n in range(1, half):
        load(2 * n, 1)
    for n in range(half):
        load(2 * n + 1, 2)
    fetch = pltpu.make_async_copy(table_in, table, t_sem)
    fetch.start()

    barrier = pltpu.get_barrier_semaphore()

    def signal(semaphore, device):
        pl.semaphore_signal(semaphore, inc=1, device_id={"tile": device}, device_id_type=pl.DeviceIdType.MESH)

    @pl.when(am_hub == 1)
    def _():
        def greet(i, carry):
            signal(barrier, lax.rem(me + i, total))
            return carry

        lax.fori_loop(1, total, greet, 0)

    @pl.when(am_hub == 0)
    def _():
        for offset in offsets:
            other = lax.rem(me + offset, total)

            @pl.when(other > me)
            def _():
                signal(barrier, other)

    expected, peers = HUBS - am_hub, 0
    for offset in offsets:
        other = lax.rem(me + offset, total)
        plain = 1 - hub_flag(other)
        expected = expected + jnp.where(other < me, plain, 0)
        peers = peers + jnp.where(other > me, plain, 0)

    def remote(src, dst, send, recv, device):
        return pltpu.make_async_remote_copy(
            src_ref=src, dst_ref=dst, send_sem=send, recv_sem=recv,
            device_id={"tile": device}, device_id_type=pl.DeviceIdType.MESH)

    flat = q.reshape(panels * levels * ct, 128)
    blocks = levels // per
    early = me < across
    late = jnp.logical_not(early)
    deferred = jnp.logical_or(early, am_hub == 1)

    def prepare_rows(parity, n):
        p = 2 * n + parity
        for block in range(blocks):
            for depth in range(DEPTH):
                x, base = depth * blocks + block, (p * levels + block * per) * ct
                s[parity, 3, n, x] = flat[pl.ds(base + depth, per, stride=ct)]
                s[parity, 1, n, x] = flat[pl.ds(base + ct - 1 - depth, per, stride=ct)]

    def finish_columns(parity, gathered):
        own[parity] = gathered.T
        for n in range(half):
            for block in range(blocks):
                base = (n * levels + block * per) * 4
                for c, (e, depth) in enumerate(((2, 1), (2, 0), (0, 0), (0, 1))):
                    s[parity, e, n, depth * blocks + block] = own[parity, pl.ds(base + c, per, stride=4)]

    def tell():
        @pl.when(am_hub == 0)
        def _():
            for offset in offsets:
                other = lax.rem(me + offset, total)

                @pl.when(other < me)
                def _():
                    signal(peer, other)

        for hub in hubs:
            @pl.when(me != hub)
            def _():
                signal(ready, hub)

    def send_seams(parity, edges, order):
        on, along = edge_state(me, parity, total, across)
        for e in edges:
            @pl.when(on[e])
            def _():
                slot = ((parity * 4 + e) * across + along[e]) * half

                def piece(i):
                    return s.at[parity, e, :, i], r.at[pl.ds(slot, half)]

                @pl.when(am_hub == 0)
                def _():
                    for i in order:
                        src, dst = piece(i)
                        remote(src, dst, send1, r_sem, hubs[i]).start()

                @pl.when(am_hub == 1)
                def _():
                    for i in order:
                        src, dst = piece(i)

                        @pl.when(me != hubs[i])
                        def _():
                            remote(src, dst, send1, r_sem, hubs[i]).start()

                        @pl.when(me == hubs[i])
                        def _():
                            pltpu.make_async_copy(src, dst, r_sem).start()

    def send_neighbours():
        @pl.when(peers > 0)
        def _():
            pl.semaphore_wait(peer, peers)

        for parity in range(2):
            on, _ = edge_state(me, parity, total, across)
            for e in range(4):
                @pl.when(jnp.logical_not(on[e]))
                def _():
                    far = (e + 2) % 4
                    remote(s.at[parity, e], h.at[parity, far], send1, h_sem,
                           lax.rem(me + steps[e], total)).start()

    for parity in range(2):
        gathered = jnp.zeros((ct, 128), jnp.float32)
        if parity == 0:
            drain(q.at[0], q_sem.at[0])
            prepare_rows(0, 0)
            gathered = gather_columns(q, 0, 0, gathered)
            drain(q.at[pl.ds(0, half - 1)], q_sem.at[1])
        else:
            drain(q.at[pl.ds(0, half)], q_sem.at[2])
        for n in range(1 - parity, half):
            prepare_rows(parity, n)
        load_fields(parity)

        @pl.when(late)
        def _():
            if parity == 0:
                pl.semaphore_wait(barrier, expected)
            send_seams(parity, (1, 3), range(HUBS))

        for n in range(1 - parity, half):
            gathered = gather_columns(q, 2 * n + parity, n, gathered)
        finish_columns(parity, gathered)

        @pl.when(late)
        def _():
            send_seams(parity, (0, 2), range(HUBS))
            if parity == 1:
                tell()

    @pl.when(early)
    def _():
        pl.semaphore_wait(barrier, expected)
        for parity in range(2):
            send_seams(parity, range(4), range(HUBS - 1, -1, -1))
        tell()

    @pl.when(jnp.logical_not(deferred))
    def _():
        send_neighbours()

    def compute(first, last):
        def one(p, carry):
            update_panel(q, east, north, coupling, u, p)
            return carry

        lax.fori_loop(first, last, one, 0)

    fetch.wait()
    seams = [(edge_tile(e, spot, across) + parity * (total // 2 + 1), parity, e, spot)
             for parity in range(2) for e in range(4) for spot in range(across)]
    seams = sorted((tile % total, *rest) for tile, *rest in seams)

    @pl.when(am_hub == 1)
    def _():
        for e in range(4):
            for p in range(panels):
                other, f, turn = table[0, e, p], table[1, e, p], table[2, e, p]
                base = (lax.rem(other, 2) * 4 + f) * across * half + other // 2
                base = jnp.where(turn == 1, base + (across - 1) * half, base)
                step = jnp.where(turn == 1, -half, half)
                for spot in range(across):
                    route[((p % 2 * 4 + e) * across + spot) * half + p // 2] = base + step * spot

    arrive(0)
    compute(0, half)

    @pl.when(deferred)
    def _():
        send_neighbours()

    @pl.when(am_hub == 1)
    def _():
        pl.semaphore_wait(ready, total - 1)
        pltpu.make_async_copy(r, r, r_sem).wait()
        place = jnp.where(me == hubs[1], 1, 0) + jnp.where(me == hubs[2], 2, 0) + jnp.where(me == hubs[3], 3, 0)
        for owner, parity, e, spot in seams:
            slot = ((parity * 4 + e) * across + spot) * half
            for n in range(half):
                d[slot + n] = r[route[slot + n]]
            src = d.at[pl.ds(slot, half)]
            dst = h.at[parity, e, :, place]
            if owner in hubs:
                @pl.when(me != owner)
                def _():
                    remote(src, dst, send2, h_sem, owner).start()

                @pl.when(me == owner)
                def _():
                    pltpu.make_async_copy(src, dst, h_sem).start()
            else:
                remote(src, dst, send2, h_sem, owner).start()

    arrive(1)
    sub = lax.broadcasted_iota(jnp.int32, (8, 128), 0)
    low, inner = sub < 4, jnp.logical_and(sub >= 2, sub < 6)
    for parity in range(2):
        north_columns = columns_of(north, parity, half)
        coupling_columns = columns_of(coupling, parity, half)
        for n in range(half):
            p = 2 * n + parity
            inverses, ratios = factors(
                lambda k: jnp.where(inner, packed_columns(coupling_columns, n * levels + k),
                                    packed_rows(coupling, p, k, low)), levels)
            for k in range(levels):
                group = n * levels + k
                coef = jnp.where(inner, packed_columns(north_columns, group), packed_rows(east, p, k, low))
                scaled = coef * inverses[k] * (-1.0 / 12.0)
                mine = packed_columns(own[parity, (group // 2) * 8:(group // 2) * 8 + 8], group % 2)
                back1, back2 = pltpu.roll(mine, 7, 0), pltpu.roll(mine, 6, 0)
                fore1, fore2 = pltpu.roll(mine, 1, 0), pltpu.roll(mine, 2, 0)
                part = jnp.where(sub == 2, back2, jnp.where(sub == 3, back2 - 8.0 * back1,
                                 jnp.where(sub == 4, 8.0 * fore1 - fore2, -fore2)))
                spot = parity * half * levels + group
                drive[spot] = scaled
                still[spot] = jnp.where(inner, part * scaled, 0.0)
                ratio[spot] = ratios[k]
                if k > 0:
                    carry[spot] = inverses[k] * below
                below = jnp.where(inner, packed_columns(coupling_columns, group), packed_rows(coupling, p, k, low))

    compute(half, panels)

    seam_edges = 0
    for parity in range(2):
        on, _ = edge_state(me, parity, total, across)
        for e in range(4):
            seam_edges = seam_edges + jnp.where(on[e], 1, 0)
    for count in range(5):
        @pl.when(seam_edges * am_hub == count)
        def _():
            drain(r.at[pl.ds(0, (8 * HUBS - count) * half)], send1)

        @pl.when(jnp.logical_and(seam_edges == count, am_hub == 1))
        def _():
            drain(d.at[pl.ds(0, (8 * across - count) * half)], send2)

    lane = lax.broadcasted_iota(jnp.int32, (levels, 128), 1)
    change[...] = jnp.zeros_like(change)
    drain(h, h_sem)
    for parity in range(2):
        on, _ = edge_state(me, parity, total, across)
        for n in range(half):
            p = 2 * n + parity
            first = (parity * half + n) * levels * 8

            def ghosts(e):
                turned = jnp.logical_and(on[e], table[2, e, p] == 1)
                found = []
                for depth in range(DEPTH):
                    rows_in = jnp.concatenate([h[parity, e, n, depth * blocks + block] for block in range(blocks)], axis=0)
                    found.append(jnp.where(turned, jnp.take_along_axis(rows_in, 127 - lane, axis=1), rows_in))
                return found

            south, east_side, north_side, west = (ghosts(e) for e in range(4))
            for spots, (above1, above2), (below1, below2) in (
                    ((2, 3, 4, 5), north_side, south), ((6, 7, 0, 1), east_side, west)):
                values = (-above1, 8.0 * above1 - above2, below2 - 8.0 * below1, below1)
                for spot, value in zip(spots, values):
                    ghost[pl.ds(first + spot, levels, stride=8)] = value
    for parity in range(2):
        for n in range(half):
            start = (parity * half + n) * levels
            partials = []
            for k in range(levels):
                at = start + k
                current = ghost[at * 8:at * 8 + 8] * drive[at] + still[at]
                if k > 0:
                    current = current + carry[at] * partials[-1]
                partials.append(current)
            solved = [partials[-1]]
            for k in range(levels - 2, -1, -1):
                solved.insert(0, partials[k] + ratio[start + k] * solved[0])
            for k in range(levels):
                rows[start + k] = solved[k]
            for k in range(0, levels, 2):
                both = jnp.where(low, pltpu.roll(solved[k], 6, 0), pltpu.roll(solved[k + 1], 2, 0))
                change[parity, (n * levels + k) * 4:(n * levels + k) * 4 + 8] = both
    for parity in range(2):
        cols[parity] = change[parity].T


def finish_kernel(u, cols, rows, result, out, out_sem):
    panels, levels, ct, _ = u.shape
    half = panels // 2
    size = 8
    wide = lax.broadcasted_iota(jnp.int32, (size, 128), 1)
    sub = lax.broadcasted_iota(jnp.int32, (size, 128), 0)
    edge = jnp.logical_or(wide < DEPTH, wide >= 128 - DEPTH)

    def store(p, block):
        part = pl.ds(block * LEVELS_AT_ONCE, LEVELS_AT_ONCE)
        return pltpu.make_async_copy(out.at[p, part], result.at[p, part], out_sem)

    for p in range(panels):
        n, parity = p // 2, p % 2
        for k in range(levels):
            group = n * levels + k
            extra = rows[parity * half * levels + group]
            for start in range(0, ct, size):
                patch = pltpu.roll(cols[parity, start:start + size], (126 - 4 * group) % 128, 1)
                value = u[p, k, start:start + size] + jnp.where(edge, patch, 0.0)
                if start == 0:
                    value = value + jnp.where(sub < DEPTH, extra, 0.0)
                if start == ct - size:
                    value = value + jnp.where(sub >= size - DEPTH, extra, 0.0)
                out[p, k, start:start + size] = value
            if k % LEVELS_AT_ONCE == LEVELS_AT_ONCE - 1:
                store(p, k // LEVELS_AT_ONCE).start()
    pltpu.make_async_copy(out, result, out_sem).wait()


def solution(mesh):
    total = mesh.shape["tile"]
    across = math.isqrt(total)

    def shards(tracer, courant_east, courant_north, diffusivity, seam_table):
        _, panels, levels, ct, _ = tracer.shape
        half, per = panels // 2, DEPTH * levels // HUBS
        strips = (2, 4, half, HUBS, per, ct)
        units = (2 * 4 * across * half, per, ct)
        packs = (panels * levels, 8, ct)
        shape = tracer.shape[1:]
        anywhere = pl.BlockSpec(memory_space=pl.ANY)
        hbm = pl.BlockSpec(memory_space=pltpu.HBM)
        whole = pl.BlockSpec(memory_space=pltpu.VMEM)
        table = jnp.transpose(seam_table, (2, 1, 0))
        plain, cols, rows = pl.pallas_call(
            functools.partial(exchange_kernel, total, across),
            out_shape=[pltpu.VMEM(dims, jnp.float32) for dims in (shape, (2, ct, ct), packs)],
            in_specs=[hbm] * 5,
            out_specs=[whole] * 3,
            scratch_shapes=[
                pltpu.SMEM(table.shape, jnp.int32),
                pltpu.SMEM(units[:1], jnp.int32),
                pltpu.VMEM(shape, jnp.float32),
                pltpu.VMEM((3,) + shape, jnp.bfloat16),
                pltpu.VMEM(strips, jnp.float32),
                pltpu.VMEM(units, jnp.float32),
                pltpu.VMEM(units, jnp.float32),
                pltpu.VMEM(strips, jnp.float32),
                pltpu.VMEM((2, ct, ct), jnp.float32),
                pltpu.VMEM(packs, jnp.float32),
                pltpu.VMEM(packs, jnp.float32),
                pltpu.VMEM(packs, jnp.float32),
                pltpu.VMEM(packs, jnp.float32),
                pltpu.VMEM((panels * levels * 8, ct), jnp.float32),
                pltpu.VMEM((2, ct, ct), jnp.float32),
                pltpu.SemaphoreType.DMA,
                pltpu.SemaphoreType.DMA((3,)),
                pltpu.SemaphoreType.DMA((2,)),
                pltpu.SemaphoreType.DMA,
                pltpu.SemaphoreType.DMA,
                pltpu.SemaphoreType.DMA,
                pltpu.SemaphoreType.DMA,
                pltpu.SemaphoreType.REGULAR,
                pltpu.SemaphoreType.REGULAR,
            ],
            compiler_params=pltpu.CompilerParams(collective_id=0, has_side_effects=True,
                                                 vmem_limit_bytes=VMEM_LIMIT),
            name="exchange",
        )(table, tracer[0], courant_east[0], courant_north[0], diffusivity[0])
        updated = pl.pallas_call(
            finish_kernel,
            out_shape=jax.ShapeDtypeStruct(shape, jnp.float32),
            in_specs=[whole] * 3,
            out_specs=anywhere,
            scratch_shapes=[pltpu.VMEM(shape, jnp.float32), pltpu.SemaphoreType.DMA],
            compiler_params=pltpu.CompilerParams(vmem_limit_bytes=VMEM_LIMIT // 2),
            name="finish",
        )(plain, cols, rows)
        return updated[None]

    placed = P(("groups", "tile"), None, None, None, None)
    return jax.shard_map(
        shards, mesh=mesh, in_specs=(placed, placed, placed, placed, P()), out_specs=placed,
        check_vma=False)
```

```python
import functools
import math

import jax
import jax.numpy as jnp
from jax import lax
from jax.experimental import pallas as pl
from jax.experimental.pallas import tpu as pltpu
from jax.sharding import PartitionSpec as P

DEPTH = 2
HUBS = 4
LEVELS_AT_ONCE = 2
VMEM_LIMIT = 59 * 1024 * 1024


def tile_of(device, parity, total):
    return lax.rem(device + total - parity * (total // 2 + 1) + total, total)


def edge_state(device, parity, total, across):
    tile = tile_of(device, parity, total)
    row, col = tile // across, lax.rem(tile, across)
    on = (col == 0, row == across - 1, col == across - 1, row == 0)
    return on, (row, col, row, col)


def hubs_of(total, across):
    middle = total // 2
    return (middle - 2 * across + 1, middle - across - 1, middle - across + 1, middle + 1)


def edge_tile(edge, spot, across):
    return (spot * across, (across - 1) * across + spot, spot * across + across - 1, spot)[edge]


def central(q, p, k, start, size):
    ct = q.shape[2]
    mid = q[p, k, start:start + size]
    none = jnp.zeros((DEPTH, 128), jnp.float32)
    if start == 0:
        ext = jnp.concatenate([none, q[p, k, 0:size + DEPTH]], axis=0)
        near = [ext[o:o + size] for o in (0, 1, 3, 4)]
    elif start + size == ct:
        ext = jnp.concatenate([q[p, k, start - DEPTH:ct], none], axis=0)
        near = [ext[o:o + size] for o in (0, 1, 3, 4)]
    else:
        near = [q[p, k, start + o:start + o + size] for o in (-2, -1, 1, 2)]
    along_i = 8.0 * (near[2] - near[1]) - (near[3] - near[0])
    along_j = 8.0 * (pltpu.roll(mid, 127, 1) - pltpu.roll(mid, 1, 1)) - (
        pltpu.roll(mid, 126, 1) - pltpu.roll(mid, 2, 1))
    return mid, along_i, along_j


def factors(coupling, levels):
    inverses, ratios, below = [], [], None
    for k in range(levels):
        here = coupling(k)
        if k == 0:
            inverse = 1.0 / (1.0 + here)
        else:
            inverse = 1.0 / ((1.0 + here) + below * (1.0 - ratios[-1]))
        inverses.append(inverse)
        ratios.append(here * inverse)
        below = here
    return inverses, ratios


def solve(forced, coupling, levels):
    ratios, partials = [], []
    for k in range(levels):
        value, here = forced(k), coupling(k)
        if k == 0:
            inverse = 1.0 / (1.0 + here)
            current = value * inverse
        else:
            inverse = 1.0 / ((1.0 + here) + below * (1.0 - ratios[-1]))
            current = (value + below * partials[-1]) * inverse
        ratios.append(here * inverse)
        partials.append(current)
        below = here
    solved = [partials[-1]]
    for k in range(levels - 2, -1, -1):
        solved.insert(0, partials[k] + ratios[k] * solved[0])
    return solved


def update_panel(q, east, north, coupling, u, p):
    _, levels, ct, _ = q.shape
    size = 16
    for start in range(0, ct, size):
        part = pl.ds(start, size)

        def forced(k):
            mid, along_i, along_j = central(q, p, k, start, size)
            return mid - (east[p, k, part].astype(jnp.float32) * along_i
                          + north[p, k, part].astype(jnp.float32) * along_j) * (1.0 / 12.0)

        solved = solve(forced, lambda k: coupling[p, k, part].astype(jnp.float32), levels)
        for k in range(levels):
            u[p, k, part] = solved[k]


def gather_columns(field, p, n, gathered):
    _, levels, ct, _ = field.shape
    lane_group = lax.broadcasted_iota(jnp.int32, (ct, 128), 1) // 4
    for k in range(levels):
        group = n * levels + k
        turned = pltpu.roll(field[p, k].astype(jnp.float32), (group * 4 + DEPTH) % 128, 1)
        gathered = jnp.where(lane_group == group, turned, gathered)
    return gathered


def columns_of(field, parity, half):
    gathered = jnp.zeros((field.shape[2], 128), jnp.float32)
    for n in range(half):
        gathered = gather_columns(field, 2 * n + parity, n, gathered)
    return gathered.T


def packed_columns(upright, group):
    pair = upright[(group // 2) * 8:(group // 2) * 8 + 8]
    return pltpu.roll(pair, 2 if group % 2 == 0 else 6, 0)


def packed_rows(field, p, k, low):
    ct = field.shape[2]
    top = field[p, k, 0:16].astype(jnp.float32)[0:8]
    bottom = field[p, k, ct - 16:ct].astype(jnp.float32)[8:16]
    return jnp.where(low, top, bottom)


def exchange_kernel(total, across, table_in, tracer, east_in, north_in, coupling_in, u, cols, rows,
                    table, route, q, fields, s, r, d, h, own, drive, carry, ratio, still, ghost, change,
                    t_sem, q_sem, c_sem, send1, r_sem, send2, h_sem, peer, ready):
    panels, levels, ct, _ = q.shape
    half = panels // 2
    per = DEPTH * levels // HUBS
    hubs = hubs_of(total, across)
    me = lax.axis_index("tile")
    steps = (total - 1, across, 1, total - across)
    offsets = sorted(set(steps))

    def hub_flag(device):
        flag = jnp.where(device == hubs[0], 1, 0)
        for hub in hubs[1:]:
            flag = flag + jnp.where(device == hub, 1, 0)
        return flag

    am_hub = hub_flag(me)

    def load(p, stage):
        pltpu.make_async_copy(tracer.at[p], q.at[p], q_sem.at[stage]).start()

    def drain(ref, sem):
        pltpu.make_async_copy(ref, ref, sem).wait()

    def load_fields(stage):
        part = pl.ds(stage * half, half)
        for i, src in enumerate((east_in, north_in, coupling_in)):
            pltpu.make_async_copy(src.at[part], fields.at[i, part], c_sem.at[stage]).start()

    def arrive(stage):
        drain(fields.at[:, pl.ds(stage * half, half)], c_sem.at[stage])

    east, north, coupling = (fields.at[i] for i in range(3))
    load(0, 0)
    for n in range(1, half):
        load(2 * n, 1)
    for n in range(half):
        load(2 * n + 1, 2)
    fetch = pltpu.make_async_copy(table_in, table, t_sem)
    fetch.start()

    barrier = pltpu.get_barrier_semaphore()

    def signal(semaphore, device):
        pl.semaphore_signal(semaphore, inc=1, device_id={"tile": device}, device_id_type=pl.DeviceIdType.MESH)

    @pl.when(am_hub == 1)
    def _():
        def greet(i, carry):
            signal(barrier, lax.rem(me + i, total))
            return carry

        lax.fori_loop(1, total, greet, 0)

    @pl.when(am_hub == 0)
    def _():
        for offset in offsets:
            other = lax.rem(me + offset, total)

            @pl.when(other > me)
            def _():
                signal(barrier, other)

    expected, peers = HUBS - am_hub, 0
    for offset in offsets:
        other = lax.rem(me + offset, total)
        plain = 1 - hub_flag(other)
        expected = expected + jnp.where(other < me, plain, 0)
        peers = peers + jnp.where(other > me, plain, 0)

    def remote(src, dst, send, recv, device):
        return pltpu.make_async_remote_copy(
            src_ref=src, dst_ref=dst, send_sem=send, recv_sem=recv,
            device_id={"tile": device}, device_id_type=pl.DeviceIdType.MESH)

    flat = q.reshape(panels * levels * ct, 128)
    blocks = levels // per
    early = me < across
    late = jnp.logical_not(early)
    deferred = jnp.logical_or(early, am_hub == 1)

    def prepare_rows(parity, n):
        p = 2 * n + parity
        for block in range(blocks):
            for depth in range(DEPTH):
                x, base = depth * blocks + block, (p * levels + block * per) * ct
                s[parity, 3, n, x] = flat[pl.ds(base + depth, per, stride=ct)]
                s[parity, 1, n, x] = flat[pl.ds(base + ct - 1 - depth, per, stride=ct)]

    def finish_columns(parity, gathered):
        own[parity] = gathered.T
        for n in range(half):
            for block in range(blocks):
                base = (n * levels + block * per) * 4
                for c, (e, depth) in enumerate(((2, 1), (2, 0), (0, 0), (0, 1))):
                    s[parity, e, n, depth * blocks + block] = own[parity, pl.ds(base + c, per, stride=4)]

    def tell():
        @pl.when(am_hub == 0)
        def _():
            for offset in offsets:
                other = lax.rem(me + offset, total)

                @pl.when(other < me)
                def _():
                    signal(peer, other)

        for hub in hubs:
            @pl.when(me != hub)
            def _():
                signal(ready, hub)

    def send_seams(parity, edges, order):
        on, along = edge_state(me, parity, total, across)
        for e in edges:
            @pl.when(on[e])
            def _():
                slot = ((parity * 4 + e) * across + along[e]) * half

                def piece(i):
                    return s.at[parity, e, :, i], r.at[pl.ds(slot, half)]

                @pl.when(am_hub == 0)
                def _():
                    for i in order:
                        src, dst = piece(i)
                        remote(src, dst, send1, r_sem, hubs[i]).start()

                @pl.when(am_hub == 1)
                def _():
                    for i in order:
                        src, dst = piece(i)

                        @pl.when(me != hubs[i])
                        def _():
                            remote(src, dst, send1, r_sem, hubs[i]).start()

                        @pl.when(me == hubs[i])
                        def _():
                            pltpu.make_async_copy(src, dst, r_sem).start()

    def send_neighbours():
        @pl.when(peers > 0)
        def _():
            pl.semaphore_wait(peer, peers)

        for parity in range(2):
            on, _ = edge_state(me, parity, total, across)
            for e in range(4):
                @pl.when(jnp.logical_not(on[e]))
                def _():
                    far = (e + 2) % 4
                    remote(s.at[parity, e], h.at[parity, far], send1, h_sem,
                           lax.rem(me + steps[e], total)).start()

    for parity in range(2):
        gathered = jnp.zeros((ct, 128), jnp.float32)
        if parity == 0:
            drain(q.at[0], q_sem.at[0])
            prepare_rows(0, 0)
            gathered = gather_columns(q, 0, 0, gathered)
            drain(q.at[pl.ds(0, half - 1)], q_sem.at[1])
        else:
            drain(q.at[pl.ds(0, half)], q_sem.at[2])
        for n in range(1 - parity, half):
            prepare_rows(parity, n)
        load_fields(parity)

        @pl.when(late)
        def _():
            if parity == 0:
                pl.semaphore_wait(barrier, expected)
            send_seams(parity, (1, 3), range(HUBS))

        for n in range(1 - parity, half):
            gathered = gather_columns(q, 2 * n + parity, n, gathered)
        finish_columns(parity, gathered)

        @pl.when(late)
        def _():
            send_seams(parity, (0, 2), range(HUBS))
            if parity == 1:
                tell()

    @pl.when(early)
    def _():
        pl.semaphore_wait(barrier, expected)
        for parity in range(2):
            send_seams(parity, range(4), range(HUBS - 1, -1, -1))
        tell()

    @pl.when(jnp.logical_not(deferred))
    def _():
        send_neighbours()

    def compute(first, last):
        def one(p, carry):
            update_panel(q, east, north, coupling, u, p)
            return carry

        lax.fori_loop(first, last, one, 0)

    fetch.wait()
    seams = [(edge_tile(e, spot, across) + parity * (total // 2 + 1), parity, e, spot)
             for parity in range(2) for e in range(4) for spot in range(across)]
    seams = sorted((tile % total, *rest) for tile, *rest in seams)

    @pl.when(am_hub == 1)
    def _():
        for e in range(4):
            for p in range(panels):
                other, f, turn = table[0, e, p], table[1, e, p], table[2, e, p]
                base = (lax.rem(other, 2) * 4 + f) * across * half + other // 2
                base = jnp.where(turn == 1, base + (across - 1) * half, base)
                step = jnp.where(turn == 1, -half, half)
                for spot in range(across):
                    route[((p % 2 * 4 + e) * across + spot) * half + p // 2] = base + step * spot

    arrive(0)
    compute(0, half)

    arrive(1)
    sub = lax.broadcasted_iota(jnp.int32, (8, 128), 0)
    low, inner = sub < 4, jnp.logical_and(sub >= 2, sub < 6)
    for parity in range(2):
        north_columns = columns_of(north, parity, half)
        coupling_columns = columns_of(coupling, parity, half)
        for n in range(half):
            p = 2 * n + parity
            inverses, ratios = factors(
                lambda k: jnp.where(inner, packed_columns(coupling_columns, n * levels + k),
                                    packed_rows(coupling, p, k, low)), levels)
            for k in range(levels):
                group = n * levels + k
                coef = jnp.where(inner, packed_columns(north_columns, group), packed_rows(east, p, k, low))
                scaled = coef * inverses[k] * (-1.0 / 12.0)
                mine = packed_columns(own[parity, (group // 2) * 8:(group // 2) * 8 + 8], group % 2)
                back1, back2 = pltpu.roll(mine, 7, 0), pltpu.roll(mine, 6, 0)
                fore1, fore2 = pltpu.roll(mine, 1, 0), pltpu.roll(mine, 2, 0)
                part = jnp.where(sub == 2, back2, jnp.where(sub == 3, back2 - 8.0 * back1,
                                 jnp.where(sub == 4, 8.0 * fore1 - fore2, -fore2)))
                spot = parity * half * levels + group
                drive[spot] = scaled
                still[spot] = jnp.where(inner, part * scaled, 0.0)
                ratio[spot] = ratios[k]
                if k > 0:
                    carry[spot] = inverses[k] * below
                below = jnp.where(inner, packed_columns(coupling_columns, group), packed_rows(coupling, p, k, low))

    @pl.when(deferred)
    def _():
        send_neighbours()

    @pl.when(am_hub == 1)
    def _():
        pl.semaphore_wait(ready, total - 1)
        pltpu.make_async_copy(r, r, r_sem).wait()
        place = jnp.where(me == hubs[1], 1, 0) + jnp.where(me == hubs[2], 2, 0) + jnp.where(me == hubs[3], 3, 0)
        for owner, parity, e, spot in seams:
            slot = ((parity * 4 + e) * across + spot) * half
            for n in range(half):
                d[slot + n] = r[route[slot + n]]
            src = d.at[pl.ds(slot, half)]
            dst = h.at[parity, e, :, place]
            if owner in hubs:
                @pl.when(me != owner)
                def _():
                    remote(src, dst, send2, h_sem, owner).start()

                @pl.when(me == owner)
                def _():
                    pltpu.make_async_copy(src, dst, h_sem).start()
            else:
                remote(src, dst, send2, h_sem, owner).start()

    compute(half, panels)

    seam_edges = 0
    for parity in range(2):
        on, _ = edge_state(me, parity, total, across)
        for e in range(4):
            seam_edges = seam_edges + jnp.where(on[e], 1, 0)
    for count in range(5):
        @pl.when(seam_edges * am_hub == count)
        def _():
            drain(r.at[pl.ds(0, (8 * HUBS - count) * half)], send1)

        @pl.when(jnp.logical_and(seam_edges == count, am_hub == 1))
        def _():
            drain(d.at[pl.ds(0, (8 * across - count) * half)], send2)

    lane = lax.broadcasted_iota(jnp.int32, (levels, 128), 1)
    change[...] = jnp.zeros_like(change)
    drain(h, h_sem)
    for parity in range(2):
        on, _ = edge_state(me, parity, total, across)
        for n in range(half):
            p = 2 * n + parity
            first = (parity * half + n) * levels * 8

            def ghosts(e):
                turned = jnp.logical_and(on[e], table[2, e, p] == 1)
                found = []
                for depth in range(DEPTH):
                    rows_in = jnp.concatenate([h[parity, e, n, depth * blocks + block] for block in range(blocks)], axis=0)
                    found.append(jnp.where(turned, jnp.take_along_axis(rows_in, 127 - lane, axis=1), rows_in))
                return found

            south, east_side, north_side, west = (ghosts(e) for e in range(4))
            for spots, (above1, above2), (below1, below2) in (
                    ((2, 3, 4, 5), north_side, south), ((6, 7, 0, 1), east_side, west)):
                values = (-above1, 8.0 * above1 - above2, below2 - 8.0 * below1, below1)
                for spot, value in zip(spots, values):
                    ghost[pl.ds(first + spot, levels, stride=8)] = value
    for parity in range(2):
        for n in range(half):
            start = (parity * half + n) * levels
            partials = []
            for k in range(levels):
                at = start + k
                current = ghost[at * 8:at * 8 + 8] * drive[at] + still[at]
                if k > 0:
                    current = current + carry[at] * partials[-1]
                partials.append(current)
            solved = [partials[-1]]
            for k in range(levels - 2, -1, -1):
                solved.insert(0, partials[k] + ratio[start + k] * solved[0])
            for k in range(levels):
                rows[start + k] = solved[k]
            for k in range(0, levels, 2):
                both = jnp.where(low, pltpu.roll(solved[k], 6, 0), pltpu.roll(solved[k + 1], 2, 0))
                change[parity, (n * levels + k) * 4:(n * levels + k) * 4 + 8] = both
    for parity in range(2):
        cols[parity] = change[parity].T


def finish_kernel(u, cols, rows, result, out, out_sem):
    panels, levels, ct, _ = u.shape
    half = panels // 2
    size = 8
    wide = lax.broadcasted_iota(jnp.int32, (size, 128), 1)
    sub = lax.broadcasted_iota(jnp.int32, (size, 128), 0)
    edge = jnp.logical_or(wide < DEPTH, wide >= 128 - DEPTH)

    def store(p, block):
        part = pl.ds(block * LEVELS_AT_ONCE, LEVELS_AT_ONCE)
        return pltpu.make_async_copy(out.at[p, part], result.at[p, part], out_sem)

    for p in range(panels):
        n, parity = p // 2, p % 2
        for k in range(levels):
            group = n * levels + k
            extra = rows[parity * half * levels + group]
            for start in range(0, ct, size):
                patch = pltpu.roll(cols[parity, start:start + size], (126 - 4 * group) % 128, 1)
                value = u[p, k, start:start + size] + jnp.where(edge, patch, 0.0)
                if start == 0:
                    value = value + jnp.where(sub < DEPTH, extra, 0.0)
                if start == ct - size:
                    value = value + jnp.where(sub >= size - DEPTH, extra, 0.0)
                out[p, k, start:start + size] = value
            if k % LEVELS_AT_ONCE == LEVELS_AT_ONCE - 1:
                store(p, k // LEVELS_AT_ONCE).start()
    pltpu.make_async_copy(out, result, out_sem).wait()


def solution(mesh):
    total = mesh.shape["tile"]
    across = math.isqrt(total)

    def shards(tracer, courant_east, courant_north, diffusivity, seam_table):
        _, panels, levels, ct, _ = tracer.shape
        half, per = panels // 2, DEPTH * levels // HUBS
        strips = (2, 4, half, HUBS, per, ct)
        units = (2 * 4 * across * half, per, ct)
        packs = (panels * levels, 8, ct)
        shape = tracer.shape[1:]
        anywhere = pl.BlockSpec(memory_space=pl.ANY)
        hbm = pl.BlockSpec(memory_space=pltpu.HBM)
        whole = pl.BlockSpec(memory_space=pltpu.VMEM)
        table = jnp.transpose(seam_table, (2, 1, 0))
        plain, cols, rows = pl.pallas_call(
            functools.partial(exchange_kernel, total, across),
            out_shape=[pltpu.VMEM(dims, jnp.float32) for dims in (shape, (2, ct, ct), packs)],
            in_specs=[hbm] * 5,
            out_specs=[whole] * 3,
            scratch_shapes=[
                pltpu.SMEM(table.shape, jnp.int32),
                pltpu.SMEM(units[:1], jnp.int32),
                pltpu.VMEM(shape, jnp.float32),
                pltpu.VMEM((3,) + shape, jnp.bfloat16),
                pltpu.VMEM(strips, jnp.float32),
                pltpu.VMEM(units, jnp.float32),
                pltpu.VMEM(units, jnp.float32),
                pltpu.VMEM(strips, jnp.float32),
                pltpu.VMEM((2, ct, ct), jnp.float32),
                pltpu.VMEM(packs, jnp.float32),
                pltpu.VMEM(packs, jnp.float32),
                pltpu.VMEM(packs, jnp.float32),
                pltpu.VMEM(packs, jnp.float32),
                pltpu.VMEM((panels * levels * 8, ct), jnp.float32),
                pltpu.VMEM((2, ct, ct), jnp.float32),
                pltpu.SemaphoreType.DMA,
                pltpu.SemaphoreType.DMA((3,)),
                pltpu.SemaphoreType.DMA((2,)),
                pltpu.SemaphoreType.DMA,
                pltpu.SemaphoreType.DMA,
                pltpu.SemaphoreType.DMA,
                pltpu.SemaphoreType.DMA,
                pltpu.SemaphoreType.REGULAR,
                pltpu.SemaphoreType.REGULAR,
            ],
            compiler_params=pltpu.CompilerParams(collective_id=0, has_side_effects=True,
                                                 vmem_limit_bytes=VMEM_LIMIT),
            name="exchange",
        )(table, tracer[0], courant_east[0], courant_north[0], diffusivity[0])
        updated = pl.pallas_call(
            finish_kernel,
            out_shape=jax.ShapeDtypeStruct(shape, jnp.float32),
            in_specs=[whole] * 3,
            out_specs=anywhere,
            scratch_shapes=[pltpu.VMEM(shape, jnp.float32), pltpu.SemaphoreType.DMA],
            compiler_params=pltpu.CompilerParams(vmem_limit_bytes=VMEM_LIMIT // 2),
            name="finish",
        )(plain, cols, rows)
        return updated[None]

    placed = P(("groups", "tile"), None, None, None, None)
    return jax.shard_map(
        shards, mesh=mesh, in_specs=(placed, placed, placed, placed, P()), out_specs=placed,
        check_vma=False)
```
